768 devices in a mesh: dom: 12 (over z), grp: 64 (over x, y, core).
Axes of the slice: x: 4, y: 8, z: 12, core: 2. Of those that a mesh axis runs over, the one named last changes fastest.
Arguments:
- master_rows: bfloat16 [64, 1536, 512], P('grp', 'dom'), may hold values from -6 to 6
- cotangent: bfloat16 [64, 1536, 512], P('grp', 'dom'), may hold values from -6 to 6
- relation_weight: bfloat16 [4, 512, 512], replicated, may hold values from -0.125 to 0.125
- self_weight: bfloat16 [512, 512], replicated, may hold values from -0.25 to 0.25
- edge_source: int32 [64, 24576], P('grp', 'dom'), may hold values from 0 to 319
- edge_target: int32 [64, 24576], P('grp', 'dom'), may hold values from 0 to 319
- edge_relation: int32 [64, 24576], P('grp', 'dom'), may hold values from 0 to 3
- send_rows: int32 [64, 2304], P('grp', 'dom'), may hold values from 0 to 127
- send_counts: int32 [64, 144], P('grp', 'dom'), may hold values from 4 to 16, as said below
Outputs:
- activation: bfloat16 [64, 1536, 512], P('grp', 'dom')
- input_grad: bfloat16 [64, 1536, 512], P('grp', 'dom')
- weight_grads: float32 [5, 512, 512], P(None, 'grp')
The draws below stay inside these ranges and needn't reach their ends.
Inputs may be any that keep to these rules, and one draw needn't show every extreme that they name: `send_counts`: on every device the count for some peer is exactly 16.
All inputs are finite; a program needn't handle non-finite values.
Results may differ from the reference program's by a relative error of at most 0.0061.
Values may be sent and summed in bfloat16 or wider, within the bound.
A program may use at most 32 MiB of HBM per device.

```python
import jax
import jax.numpy as jnp
from jax import lax

D = 512
REL = 4
MAST = 128
CAP = 16
EDGES = 2048
ROWS = 320
N_DOM = 12
N_GRP = 64


def draw_send_counts(key, part):
    key_a, key_b = jax.random.split(jax.random.fold_in(key, 17))
    halvings = jax.random.randint(key_a, (N_GRP, N_DOM, N_DOM), 0, 3)
    counts = jnp.right_shift(jnp.full((N_GRP, N_DOM, N_DOM), CAP, jnp.int32), halvings)
    busiest = jax.random.randint(key_b, (N_GRP, N_DOM, 1), 0, N_DOM)
    counts = jnp.where(jnp.arange(N_DOM)[None, None, :] == busiest, CAP, counts)
    return counts.reshape(N_GRP, N_DOM * N_DOM).astype(jnp.int32)


def touch_ends(result, rng, least, top_value):
    shape = result.shape
    place = [jax.random.randint(jax.random.fold_in(rng, axis), (), 0, shape[axis]) for axis in range(len(shape))]
    result = result.at[tuple(place)].set(least)
    longest = shape.index(max(shape))
    place[longest] = (place[longest] + 1) % shape[longest]
    return result.at[tuple(place)].set(top_value)


def steps_of(rng, extent, cuts, smallest, top_value):
    def one(axis_at, blocks):
        heights = jax.random.uniform(jax.random.fold_in(jax.random.fold_in(rng, 6), axis_at), (blocks,), jnp.float32, smallest / len(cuts), top_value / len(cuts))
        return jnp.repeat(jnp.exp(heights), extent[axis_at] // blocks).reshape((-1,) + (1,) * (len(extent) - axis_at - 1))

    level = one(*cuts[0])
    for cut in cuts[1:]:
        level = level * one(*cut)
    return level


def bell_draw(own_key, dims, spread, limit, shards=(), held_as=jnp.bfloat16):
    array = spread * jax.random.normal(own_key, dims, jnp.float32)
    if shards:
        array = array * steps_of(own_key, dims, shards, -0.22, 0.18)
    return jnp.clip(array, -limit, limit).astype(held_as)


def setup_inputs(seed: int = 0) -> dict:
    seeds = jax.random.split(jax.random.key(seed), 10)
    master_rows = bell_draw(seeds[0], (N_GRP, N_DOM * MAST, D), 1.0, 6.0, ((0, 64), (1, 12)))
    cotangent = bell_draw(seeds[1], (N_GRP, N_DOM * MAST, D), 1.0, 6.0, ((0, 64), (1, 12)))
    relation_weight = bell_draw(seeds[2], (REL, D, D), (4 * D) ** -0.5, 0.125)
    self_weight = bell_draw(seeds[3], (D, D), D ** -0.5, 0.25)
    edge_source = touch_ends(jax.random.randint(seeds[4], (N_GRP, N_DOM * EDGES), 0, ROWS), jax.random.fold_in(seeds[4], 1), 0, ROWS - 1).astype(jnp.int32)
    edge_target = touch_ends(jax.random.randint(seeds[5], (N_GRP, N_DOM * EDGES), 0, ROWS), jax.random.fold_in(seeds[5], 1), 0, ROWS - 1).astype(jnp.int32)
    edge_relation = touch_ends(jax.random.randint(seeds[6], (N_GRP, N_DOM * EDGES), 0, REL), jax.random.fold_in(seeds[6], 1), 0, REL - 1).astype(jnp.int32)
    send_rows = touch_ends(jax.random.randint(seeds[7], (N_GRP, N_DOM * N_DOM * CAP), 0, MAST), jax.random.fold_in(seeds[7], 1), 0, MAST - 1).astype(jnp.int32)
    send_counts = draw_send_counts(jax.random.fold_in(seeds[9], 71), 0)
    return dict(master_rows=master_rows, cotangent=cotangent, relation_weight=relation_weight, self_weight=self_weight, edge_source=edge_source, edge_target=edge_target, edge_relation=edge_relation, send_rows=send_rows, send_counts=send_counts)


def aggregate(table, gather_index, segment_index):
    terms = table[gather_index].astype(jnp.float32)
    summed = jax.ops.segment_sum(terms, segment_index, num_segments=REL * ROWS)
    return summed.reshape(REL, ROWS, D).astype(jnp.bfloat16)


def reference(master_rows, cotangent, relation_weight, self_weight, edge_source, edge_target, edge_relation, send_rows, send_counts):
    weights = relation_weight.astype(jnp.float32)
    masters = master_rows.reshape(N_GRP, N_DOM, MAST, D)
    cotan = cotangent.reshape(N_GRP, N_DOM, MAST, D)
    slots = send_rows.reshape(N_GRP, N_DOM, N_DOM * CAP)
    counts = send_counts.reshape(N_GRP, N_DOM, N_DOM)
    valid = (jnp.arange(CAP)[None, None, None, :] < counts[..., None]).reshape(N_GRP, N_DOM, N_DOM * CAP)
    sources = edge_source.reshape(N_GRP * N_DOM, EDGES)
    targets = edge_target.reshape(N_GRP * N_DOM, EDGES)
    relations = edge_relation.reshape(N_GRP * N_DOM, EDGES)

    def pick(table, index):
        return table[index]

    def pull(table):
        picked = jax.vmap(jax.vmap(pick))(table, slots)
        picked = jnp.where(valid[..., None], picked, jnp.zeros_like(picked))
        picked = picked.reshape(N_GRP, N_DOM, N_DOM, CAP, D).transpose(0, 2, 1, 3, 4).reshape(N_GRP, N_DOM, N_DOM * CAP, D)
        return jnp.concatenate([table, picked], axis=2)

    def add_rows(terms, index):
        return jax.ops.segment_sum(terms, index, num_segments=MAST)

    def push(parts, own):
        moved = parts.reshape(N_GRP, N_DOM, N_DOM, CAP, D).transpose(0, 2, 1, 3, 4).reshape(N_GRP, N_DOM, N_DOM * CAP, D)
        terms = jnp.where(valid[..., None], moved.astype(jnp.float32), 0.0)
        return own + jax.vmap(jax.vmap(add_rows))(terms, slots)

    table = pull(masters).reshape(N_GRP * N_DOM, ROWS, D)
    flat_masters = masters.reshape(N_GRP * N_DOM, MAST, D)

    def forward_device(inputs):
        rows, master, source, target, relation = inputs
        aggregated = aggregate(rows, source, relation * ROWS + target)
        partial_value = jnp.einsum("rnd,rde->ne", aggregated.astype(jnp.float32), weights)
        own = partial_value[:MAST] + jnp.dot(master, self_weight, preferred_element_type=jnp.float32)
        return own, partial_value[MAST:].astype(jnp.bfloat16)

    own, mirror_part = lax.map(forward_device, (table, flat_masters, sources, targets, relations))
    z_value = push(mirror_part.reshape(N_GRP, N_DOM, N_DOM * CAP, D), own.reshape(N_GRP, N_DOM, MAST, D))
    activation = jax.nn.silu(z_value).astype(jnp.bfloat16)
    sigmoid_z = jax.nn.sigmoid(z_value)
    grad_z = (cotan.astype(jnp.float32) * sigmoid_z * (1.0 + z_value * (1.0 - sigmoid_z))).astype(jnp.bfloat16)
    grad_table = pull(grad_z).reshape(N_GRP * N_DOM, ROWS, D)
    flat_grad = grad_z.reshape(N_GRP * N_DOM, MAST, D)

    def backward_device(total, inputs):
        rows, master, grad_rows, grad_master, source, target, relation = inputs
        aggregated = aggregate(rows, source, relation * ROWS + target)
        relation_grad = jnp.einsum("rnd,ne->rde", aggregated.astype(jnp.float32), grad_rows.astype(jnp.float32))
        self_grad = jnp.dot(master.T, grad_master, preferred_element_type=jnp.float32)
        back = aggregate(grad_rows, target, relation * ROWS + source)
        back_partial = jnp.einsum("rne,rde->nd", back.astype(jnp.float32), weights)
        back_own = back_partial[:MAST] + jnp.dot(grad_master, self_weight.T, preferred_element_type=jnp.float32)
        total = total + jnp.concatenate([relation_grad, self_grad[None]], axis=0)
        return total, (back_own, back_partial[MAST:].astype(jnp.bfloat16))

    start = jnp.zeros((REL + 1, D, D), jnp.float32)
    weight_grads, (back_own, back_mirror) = lax.scan(backward_device, start, (table, flat_masters, grad_table, flat_grad, sources, targets, relations))
    input_grad = push(back_mirror.reshape(N_GRP, N_DOM, N_DOM * CAP, D), back_own.reshape(N_GRP, N_DOM, MAST, D))
    activation = activation.reshape(N_GRP, N_DOM * MAST, D)
    input_grad = input_grad.astype(jnp.bfloat16).reshape(N_GRP, N_DOM * MAST, D)
    return activation, input_grad, weight_grads
```

```python
import functools

import jax
import jax.numpy as jnp
from jax import lax
from jax.experimental import pallas as pl
from jax.experimental.pallas import tpu as pltpu
from jax.sharding import Mesh
from jax.sharding import PartitionSpec as P

GRP = ("grp_0", "grp_1", "grp_2")
MESH = pl.DeviceIdType.MESH
F32 = jnp.float32
BF16 = jnp.bfloat16


def dot(a, b):
    return jnp.dot(a, b, preferred_element_type=F32)


def dot_nt(a, b):
    return lax.dot_general(a, b, (((1,), (1,)), ((), ())), preferred_element_type=F32)


def nearest_last(n):
    return sorted(range(1, n), key=lambda k: (-min(k, n - k), k))


def kernel(
    nz, ny, cap,
    counts_hbm, masters_hbm, cotan_hbm, source_hbm, target_hbm, relation_hbm, slots_hbm, relw_hbm, selfw_hbm,
    act_ref, ingrad_ref, wgrad_ref,
    counts, cotan, source, target, relation, slots, relw, selfw, one_hot, adj, adj_t, place, pick, table, agg, agg_t,
    psend, qsend, qrecv, own, gsend, gtab, back, bown, bsend, brecv, csend, crecv, lg, xs, xr, xt, ysend, ymine, yr,
    zsend, zrecv, zown, wrecv,
    in_sem, s_pull, r_pull, s_push, r_push, s_gpull, r_gpull, s_back, r_back, s_core, r_core, s_x, r_x, s_y, r_y,
    s_z, r_z, s_w, r_w,
):
    z = lax.axis_index("dom")
    x = lax.axis_index("grp_0")
    y = lax.axis_index("grp_1")
    c = lax.axis_index("grp_2")
    nx = 4
    rel = relw.shape[0]
    width = relw.shape[1]
    half = width // 2
    mast = cotan.shape[0]
    rows = table.shape[0]
    mirrors = rows - mast
    piece = width // (nx * ny * 2)
    ring = nearest_last(nz)
    yring = nearest_last(ny)
    sent = []

    def zp(k):
        return lax.rem(z + k, nz)

    def send(copy):
        copy.start()
        sent.append(copy)

    def remote(src, dst, send_sem, recv_sem, **device):
        return pltpu.make_async_remote_copy(
            src_ref=src, dst_ref=dst, send_sem=send_sem, recv_sem=recv_sem, device_id=device, device_id_type=MESH
        )

    barrier = pltpu.get_barrier_semaphore()
    met = [{"dom": zp(k)} for k in ring] + [{"grp_1": lax.rem(y + k, ny)} for k in yring]
    met += [{"grp_0": lax.rem(x + k, nx)} for k in (1, 3)] + [{"grp_2": 1 - c}]
    for device in met:
        pl.semaphore_signal(barrier, inc=1, device_id=device, device_id_type=MESH)

    brought = (
        (counts_hbm, counts), (slots_hbm, slots), (masters_hbm.at[0], table.at[:mast]), (target_hbm, target),
        (source_hbm, source), (relation_hbm, relation), (relw_hbm, relw), (selfw_hbm, selfw),
        (cotan_hbm.at[0], cotan),
    )
    inputs = [pltpu.make_async_copy(a, b, in_sem.at[i]) for i, (a, b) in enumerate(brought)]
    for copy in inputs:
        copy.start()
    for copy in inputs[:2]:
        copy.wait()

    lane = lax.broadcasted_iota(jnp.int32, (1, mirrors), 1)
    limit = jnp.zeros((1, mirrors), jnp.int32)
    for p in range(nz):
        limit = jnp.where((lane >= p * cap) & (lane < (p + 1) * cap), counts[0, p] + p * cap, limit)
    named = jnp.where(lane < limit, slots[...], -1)
    row = lax.broadcasted_iota(jnp.int32, (mast, mirrors), 0)
    placement = jnp.where(row == named, 1.0, 0.0)
    place[...] = placement.astype(BF16)
    pick[...] = placement.T.astype(BF16)

    inputs[2].wait()
    psend[...] = dot(pick[...], table[:mast, :]).astype(BF16).reshape(nz, cap, width)

    def mirror_rows():
        return pl.ds(pl.multiple_of(mast + z * cap, cap), cap)

    def pull(k):
        return remote(psend.at[zp(k)], table.at[mirror_rows(), :], s_pull.at[k], r_pull.at[k], dom=zp(k))

    pl.semaphore_wait(barrier, len(met))
    for k in ring:
        send(pull(k))
    table[mirror_rows(), :] = psend[z]

    for copy in inputs[3:6]:
        copy.wait()
    row = lax.broadcasted_iota(jnp.int32, (rows, source.shape[1]), 0)

    def counted(dst, first, second):
        one_hot[...] = jnp.where(row == second, 1.0, 0.0).astype(BF16)

        @pl.loop(0, rel)
        def _(r):
            mine = jnp.where(relation[...] == r, first, -1)
            hot = jnp.where(row == mine, 1.0, 0.0).astype(BF16)
            dst[pl.ds(pl.multiple_of(r * rows, rows), rows), :] = dot_nt(hot, one_hot[...]).astype(BF16)

    counted(adj, target[...], source[...])
    for copy in inputs[6:]:
        copy.wait()

    for k in ring:
        pull(k).wait_recv()
    agg[...] = dot(adj[...], table[...]).astype(BF16)

    def push(h, k):
        return remote(qsend.at[h, zp(k)], qrecv.at[h, z], s_push.at[h, k], r_push.at[h, k], dom=zp(k))

    for h in (0, 1):
        cols = slice(h * half, (h + 1) * half)
        part = dot(agg[mast:rows, :], relw[0, :, cols])
        for r in range(1, rel):
            part += dot(agg[r * rows + mast : (r + 1) * rows, :], relw[r, :, cols])
        qsend[h] = part.astype(BF16).reshape(nz, cap, half)
        qrecv[h, z] = qsend[h, z]
        for k in ring:
            send(push(h, k))

    for h in (0, 1):
        cols = slice(h * half, (h + 1) * half)
        part = dot(table[:mast, :], selfw[:, cols])
        for r in range(rel):
            part += dot(agg[r * rows : r * rows + mast, :], relw[r, :, cols])
        own[h] = part

    def transposed(values):
        turned = values.astype(F32).T.reshape(nx * ny, 2, piece, values.shape[0])
        return [turned[:, core].reshape(half, values.shape[0]).astype(BF16) for core in (0, 1)]

    for r in range(rel):
        for core, values in enumerate(transposed(agg[r * rows : (r + 1) * rows, :])):
            agg_t[r, core] = values
    for core, values in enumerate(transposed(table[:mast, :])):
        agg_t[rel, core, :, :mast] = values

    counted(adj_t, source[...], target[...])

    def gpull(h, k):
        return remote(gsend.at[h, zp(k)], gtab.at[h, mirror_rows(), :], s_gpull.at[h, k], r_gpull.at[h, k], dom=zp(k))

    for h in (0, 1):
        for k in ring:
            push(h, k).wait_recv()
        cols = slice(h * half, (h + 1) * half)
        value = own[h] + dot(place[...], qrecv[h].reshape(mirrors, half))
        gate = 1.0 / (1.0 + jnp.exp(-value))
        grad = cotan[:, cols].astype(F32) * gate * (1.0 + value * (1.0 - gate))
        gtab[h, :mast, :] = grad.astype(BF16)
        gsend[h] = dot(pick[...], gtab[h, :mast, :]).astype(BF16).reshape(nz, cap, half)
        for k in ring:
            send(gpull(h, k))
        gtab[h, mirror_rows(), :] = gsend[h, z]
        act_ref[0, :, cols] = (value * gate).astype(BF16)

    def to_core(h, r):
        return remote(csend.at[h, r], crecv.at[h, r], s_core.at[h, r], r_core.at[h, r], grp_2=1 - c)

    def local(h, r):
        seen = mast if r == rel else rows
        csend[h, r] = dot(agg_t[r, 1 - c, :, :seen], gtab[h, :seen, :]).astype(BF16)
        send(to_core(h, r))
        lg[h, r] = dot(agg_t[r, c, :, :seen], gtab[h, :seen, :])

    mrow = half // nx
    quarter = mrow // 2

    def block(owner, part):
        return pl.ds(pl.multiple_of(lax.rem(owner, nx) * mrow + part * quarter, quarter), quarter)

    def along_x(h, r, m):
        to, src = (
            (1, xs.at[h, r, block(x + 1, 1), :]),
            (1, xs.at[h, r, block(x + 2, 0), :]),
            (3, xs.at[h, r, block(x + 3, 0), :]),
            (3, xs.at[h, r, block(x + 2, 1), :]),
            (1, xt.at[h, r, 0]),
            (3, xt.at[h, r, 1]),
        )[m]
        return remote(src, xr.at[h, r, m], s_x.at[h, r, m], r_x.at[h, r, m], grp_0=lax.rem(x + to, nx))

    def first_x(h, r):
        to_core(h, r).wait_recv()
        lg[h, r] = lg[h, r] + crecv[h, r].astype(F32)
        xs[h, r] = lg[h, r].astype(BF16)
        for m in (1, 3, 0, 2):
            send(along_x(h, r, m))

    def second_x(h, r):
        along_x(h, r, 1).wait_recv()
        xt[h, r, 0] = (lg[h, r, block(x + 1, 0), :] + xr[h, r, 1].astype(F32)).astype(BF16)
        send(along_x(h, r, 4))
        along_x(h, r, 3).wait_recv()
        xt[h, r, 1] = (lg[h, r, block(x + 3, 1), :] + xr[h, r, 3].astype(F32)).astype(BF16)
        send(along_x(h, r, 5))

    def along_y(h, r, k):
        to = lax.rem(y + k, ny)
        return remote(ysend.at[h, r, to], yr.at[h, r, k], s_y.at[h, r, k], r_y.at[h, r, k], grp_1=to)

    def over_y(h, r):
        for m in (2, 4, 0, 5):
            along_x(h, r, m).wait_recv()
        ymine[h, r, :quarter, :] = lg[h, r, block(x, 0), :] + xr[h, r, 2].astype(F32) + xr[h, r, 4].astype(F32)
        ymine[h, r, quarter:, :] = lg[h, r, block(x, 1), :] + xr[h, r, 0].astype(F32) + xr[h, r, 5].astype(F32)
        ysend[h, r] = ymine[h, r].reshape(ny, piece, half).astype(BF16)
        for k in yring:
            send(along_y(h, r, k))

    parts = 2 * (rel + 1)
    held = -(-parts // nz)

    def along_z(q):
        k = lax.rem(q - z + 2 * nz, nz)
        return remote(zsend.at[q], zrecv.at[q // nz, k], s_z.at[q], r_z.at[q // nz, k], dom=q % nz)

    def over_z(h, r):
        q = 2 * r + h
        total = ymine[h, r, pl.ds(pl.multiple_of(y * piece, piece), piece), :]
        for k in yring:
            along_y(h, r, k).wait_recv()
            total += yr[h, r, k].astype(F32)
        zsend[q] = total

        @pl.when(z != q % nz)
        def _():
            along_z(q).start()

    def units(h):
        return [(h, r) for r in range(rel)]

    first = [(0, rel), (1, rel)]
    for u in first:
        local(*u)
    for u in first:
        first_x(*u)

    for k in ring:
        gpull(0, k).wait_recv()
    for u in units(0):
        local(*u)
    for u in units(0):
        first_x(*u)
    for u in first:
        second_x(*u)

    for k in ring:
        gpull(1, k).wait_recv()
    for u in units(1):
        local(*u)
    for u in units(1):
        first_x(*u)
    for u in first:
        over_y(*u)
    for u in units(0):
        second_x(*u)

    for h in (0, 1):
        back[:, h * half : (h + 1) * half] = dot(adj_t[...], gtab[h]).astype(BF16)
    part = dot_nt(back[mast:rows, :], relw[0])
    for r in range(1, rel):
        part += dot_nt(back[r * rows + mast : (r + 1) * rows, :], relw[r])
    bsend[...] = part.astype(BF16).reshape(nz, cap, width)
    brecv[z] = bsend[z]

    def bpush(k):
        return remote(bsend.at[zp(k)], brecv.at[z], s_back.at[k], r_back.at[k], dom=zp(k))

    for k in ring:
        send(bpush(k))

    for u in units(0):
        over_y(*u)
    for u in units(1):
        second_x(*u)
    for u in first:
        over_z(*u)

    part = dot_nt(gtab[0, :mast, :], selfw[:, :half]) + dot_nt(gtab[1, :mast, :], selfw[:, half:])
    for r in range(rel):
        part += dot_nt(back[r * rows : r * rows + mast, :], relw[r])
    bown[...] = part

    for u in units(1):
        over_y(*u)
    for u in units(0):
        over_z(*u)

    for k in ring:
        bpush(k).wait_recv()
    ingrad_ref[0] = (bown[...] + dot(place[...], brecv[...].reshape(mirrors, width))).astype(BF16)

    for u in units(1):
        over_z(*u)

    def shared(i, k):
        q = z + i * nz
        return remote(zown.at[i], wrecv.at[q], s_w.at[i, k], r_w.at[q], dom=zp(k))

    for i in range(held):
        q = z + i * nz

        @pl.when(q < parts)
        def _():
            total = zsend[q]
            for k in range(1, nz):
                remote(zsend.at[0], zrecv.at[i, k], s_z.at[0], r_z.at[i, k], dom=zp(1)).wait_recv()
                total += zrecv[i, k]
            zown[i] = total
            for k in ring:
                shared(i, k).start()
            wrecv[q] = total

    for q in range(parts):
        @pl.when(z != q % nz)
        def _():
            remote(zown.at[0], wrecv.at[q], s_w.at[0, 0], r_w.at[q], dom=zp(1)).wait_recv()

        h = q % 2
        wgrad_ref[q // 2, :, h * half : (h + 1) * half] = wrecv[q]

    for copy in sent:
        copy.wait_send()
    for q in range(parts):
        @pl.when(z != q % nz)
        def _():
            along_z(q).wait_send()
    for i in range(held):
        @pl.when(z + i * nz < parts)
        def _():
            for k in ring:
                shared(i, k).wait_send()


def handed_on(*refs):
    half = len(refs) // 2
    for a, b in zip(refs[:half], refs[half:]):
        b[...] = a[...]


def per_device(
    master_rows, cotangent, relation_weight, self_weight, edge_source, edge_target, edge_relation, send_rows,
    send_counts,
):
    nz = lax.axis_size("dom")
    ny = lax.axis_size("grp_1")
    rel, width = relation_weight.shape[:2]
    mast = master_rows.shape[1]
    mirrors = send_rows.shape[1]
    cap = mirrors // nz
    rows = mast + mirrors
    edges = edge_source.shape[1]
    half = width // 2
    mrow = half // 4
    piece = width // (4 * ny * 2)
    parts = 2 * (rel + 1)
    held = -(-parts // nz)
    vmem = pl.BlockSpec(memory_space=pltpu.VMEM)
    hbm = pl.BlockSpec(memory_space=pl.ANY)
    dma = pltpu.SemaphoreType.DMA
    scratch = [
        pltpu.SMEM((1, nz), jnp.int32),
        pltpu.VMEM((mast, width), BF16),
        pltpu.VMEM((1, edges), jnp.int32),
        pltpu.VMEM((1, edges), jnp.int32),
        pltpu.VMEM((1, edges), jnp.int32),
        pltpu.VMEM((1, mirrors), jnp.int32),
        pltpu.VMEM((rel, width, width), BF16),
        pltpu.VMEM((width, width), BF16),
        pltpu.VMEM((rows, edges), BF16),
        pltpu.VMEM((rel * rows, rows), BF16),
        pltpu.VMEM((rel * rows, rows), BF16),
        pltpu.VMEM((mast, mirrors), BF16),
        pltpu.VMEM((mirrors, mast), BF16),
        pltpu.VMEM((rows, width), BF16),
        pltpu.VMEM((rel * rows, width), BF16),
        pltpu.VMEM((rel + 1, 2, half, rows), BF16),
        pltpu.VMEM((nz, cap, width), BF16),
        pltpu.VMEM((2, nz, cap, half), BF16),
        pltpu.VMEM((2, nz, cap, half), BF16),
        pltpu.VMEM((2, mast, half), F32),
        pltpu.VMEM((2, nz, cap, half), BF16),
        pltpu.VMEM((2, rows, half), BF16),
        pltpu.VMEM((rel * rows, width), BF16),
        pltpu.VMEM((mast, width), F32),
        pltpu.VMEM((nz, cap, width), BF16),
        pltpu.VMEM((nz, cap, width), BF16),
        pltpu.VMEM((2, rel + 1, half, half), BF16),
        pltpu.VMEM((2, rel + 1, half, half), BF16),
        pltpu.VMEM((2, rel + 1, half, half), F32),
        pltpu.VMEM((2, rel + 1, half, half), BF16),
        pltpu.VMEM((2, rel + 1, 6, mrow // 2, half), BF16),
        pltpu.VMEM((2, rel + 1, 2, mrow // 2, half), BF16),
        pltpu.VMEM((2, rel + 1, ny, piece, half), BF16),
        pltpu.VMEM((2, rel + 1, mrow, half), F32),
        pltpu.VMEM((2, rel + 1, ny, piece, half), BF16),
        pltpu.VMEM((parts, piece, half), F32),
        pltpu.VMEM((held, nz, piece, half), F32),
        pltpu.VMEM((held, piece, half), F32),
        pltpu.VMEM((parts, piece, half), F32),
        dma((9,)),
        dma((nz,)), dma((nz,)),
        dma((2, nz)), dma((2, nz)),
        dma((2, nz)), dma((2, nz)),
        dma((nz,)), dma((nz,)),
        dma((2, rel + 1)), dma((2, rel + 1)),
        dma((2, rel + 1, 6)), dma((2, rel + 1, 6)),
        dma((2, rel + 1, ny)), dma((2, rel + 1, ny)),
        dma((parts,)), dma((held, nz)),
        dma((held, nz)), dma((parts,)),
    ]
    out_shape = (
        jax.ShapeDtypeStruct((1, mast, width), BF16),
        jax.ShapeDtypeStruct((1, mast, width), BF16),
        jax.ShapeDtypeStruct((rel + 1, piece, width), F32),
    )
    results = pl.pallas_call(
        functools.partial(kernel, nz, ny, cap),
        out_shape=tuple(pltpu.VMEM(o.shape, o.dtype) for o in out_shape),
        in_specs=[hbm] * 9,
        out_specs=(vmem, vmem, vmem),
        scratch_shapes=scratch,
        compiler_params=pltpu.CompilerParams(
            collective_id=0, has_side_effects=True, vmem_limit_bytes=56 * 1024 * 1024
        ),
        name="graph_conv_step",
    )(
        send_counts, master_rows, cotangent, edge_source, edge_target, edge_relation, send_rows, relation_weight,
        self_weight,
    )
    return pl.pallas_call(
        handed_on,
        out_shape=out_shape,
        in_specs=[vmem] * 3,
        out_specs=(vmem, vmem, vmem),
        compiler_params=pltpu.CompilerParams(vmem_limit_bytes=4 * 1024 * 1024),
        name="handed_on",
    )(*results)


def solution(mesh):
    devices = mesh.devices.shape[1]
    finer = Mesh(
        mesh.devices.reshape(mesh.shape["dom"], 4, devices // 8, 2), ("dom", "grp_0", "grp_1", "grp_2")
    )
    in_specs = (
        P(GRP, "dom", None),
        P(GRP, "dom", None),
        P(),
        P(),
        P(GRP, "dom"),
        P(GRP, "dom"),
        P(GRP, "dom"),
        P(GRP, "dom"),
        P(GRP, "dom"),
    )
    out_specs = (P(GRP, "dom", None), P(GRP, "dom", None), P(None, GRP, None))
    return jax.shard_map(per_device, mesh=finer, in_specs=in_specs, out_specs=out_specs, check_vma=False)
```

```python
import functools

import jax
import jax.numpy as jnp
from jax import lax
from jax.experimental import pallas as pl
from jax.experimental.pallas import tpu as pltpu
from jax.sharding import Mesh
from jax.sharding import PartitionSpec as P

GRP = ("grp_0", "grp_1", "grp_2")
MESH = pl.DeviceIdType.MESH
NX = 4
GROUP = 4
F32 = jnp.float32
BF16 = jnp.bfloat16


def dot(a, b):
    return jnp.dot(a, b, preferred_element_type=F32)


def dot_nt(a, b):
    return lax.dot_general(a, b, (((1,), (1,)), ((), ())), preferred_element_type=F32)


def nearest_last(n):
    return sorted(range(1, n), key=lambda k: (-min(k, n - k), k))


def kernel(
    nz, ny, cap,
    counts_hbm, masters_hbm, cotan_hbm, source_hbm, target_hbm, relation_hbm, slots_hbm, relw_hbm, selfw_hbm,
    act_ref, ingrad_ref, wgrad_ref,
    counts, cotan, source, target, relation, slots, relw, selfw, one_hot, adj, adj_t, place, pick, table, agg, agg_t,
    psend, qsend, qrecv, own, gsend, gtab, back, bown, bsend, brecv, csend, crecv, lg, xs, xr, ysend, ymine, yr,
    zmine, zsend, zrecv, zown, wrecv,
    in_sem, s_pull, r_pull, s_push, r_push, s_gpull, r_gpull, s_back, r_back, s_core, r_core, s_x, r_x, s_y, r_y,
    s_z, r_z, s_w, r_w,
):
    z = lax.axis_index("dom")
    x = lax.axis_index("grp_0")
    y = lax.axis_index("grp_1")
    c = lax.axis_index("grp_2")
    nx = NX
    rel = relw.shape[0]
    width = relw.shape[1]
    half = width // 2
    slab = width // 4
    mast = cotan.shape[0]
    rows = table.shape[0]
    mirrors = rows - mast
    piece = width // (nx * ny * 2)
    ring = nearest_last(nz)
    yring = nearest_last(ny)
    sent = []

    def zp(k):
        return lax.rem(z + k, nz)

    def send(copy):
        copy.start()
        sent.append(copy)

    def remote(src, dst, send_sem, recv_sem, **device):
        return pltpu.make_async_remote_copy(
            src_ref=src, dst_ref=dst, send_sem=send_sem, recv_sem=recv_sem, device_id=device, device_id_type=MESH
        )

    barrier = pltpu.get_barrier_semaphore()
    met = [{"dom": zp(k)} for k in ring] + [{"grp_1": lax.rem(y + k, ny)} for k in yring]
    met += [{"grp_0": lax.rem(x + k, nx)} for k in range(1, nx)] + [{"grp_2": 1 - c}]
    for device in met:
        pl.semaphore_signal(barrier, inc=1, device_id=device, device_id_type=MESH)

    brought = (
        (counts_hbm, counts), (slots_hbm, slots), (masters_hbm.at[0], table.at[:mast]), (target_hbm, target),
        (source_hbm, source), (relation_hbm, relation), (relw_hbm, relw), (selfw_hbm, selfw),
        (cotan_hbm.at[0], cotan),
    )
    inputs = [pltpu.make_async_copy(a, b, in_sem.at[i]) for i, (a, b) in enumerate(brought)]
    for copy in inputs:
        copy.start()
    for copy in inputs[:2]:
        copy.wait()

    lane = lax.broadcasted_iota(jnp.int32, (1, mirrors), 1)
    limit = jnp.zeros((1, mirrors), jnp.int32)
    for p in range(nz):
        limit = jnp.where((lane >= p * cap) & (lane < (p + 1) * cap), counts[0, p] + p * cap, limit)
    named = jnp.where(lane < limit, slots[...], -1)
    row = lax.broadcasted_iota(jnp.int32, (mast, mirrors), 0)
    placement = jnp.where(row == named, 1.0, 0.0)
    place[...] = placement.astype(BF16)
    pick[...] = placement.T.astype(BF16)

    inputs[2].wait()
    psend[...] = dot(pick[...], table[:mast, :]).astype(BF16).reshape(nz, cap, width)

    def mirror_rows():
        return pl.ds(pl.multiple_of(mast + z * cap, cap), cap)

    def pull(k):
        return remote(psend.at[zp(k)], table.at[mirror_rows(), :], s_pull.at[k], r_pull.at[k], dom=zp(k))

    pl.semaphore_wait(barrier, len(met))
    for k in ring:
        send(pull(k))
    table[mirror_rows(), :] = psend[z]

    for copy in inputs[3:6]:
        copy.wait()
    row = lax.broadcasted_iota(jnp.int32, (rows, source.shape[1]), 0)

    def counted(dst, first, second):
        one_hot[...] = jnp.where(row == second, 1.0, 0.0).astype(BF16)

        @pl.loop(0, rel)
        def _(r):
            mine = jnp.where(relation[...] == r, first, -1)
            hot = jnp.where(row == mine, 1.0, 0.0).astype(BF16)
            dst[pl.ds(pl.multiple_of(r * rows, rows), rows), :] = dot_nt(hot, one_hot[...]).astype(BF16)

    counted(adj, target[...], source[...])
    for copy in inputs[6:]:
        copy.wait()

    for k in ring:
        pull(k).wait_recv()
    for r in range(rel):
        some = slice(r * rows + mast, (r + 1) * rows)
        agg[some, :] = dot(adj[some, :], table[...]).astype(BF16)

    def push(b, k):
        return remote(qsend.at[b, zp(k)], qrecv.at[b, z], s_push.at[b, k], r_push.at[b, k], dom=zp(k))

    for h in (0, 1):
        cols = slice(h * half, (h + 1) * half)
        part = dot(agg[mast:rows, :], relw[0, :, cols])
        for r in range(1, rel):
            part += dot(agg[r * rows + mast : (r + 1) * rows, :], relw[r, :, cols])
        for b in (2 * h, 2 * h + 1):
            qsend[b] = part[:, (b % 2) * slab : (b % 2 + 1) * slab].astype(BF16).reshape(nz, cap, slab)
            qrecv[b, z] = qsend[b, z]
            for k in ring:
                send(push(b, k))

    for r in range(rel):
        some = slice(r * rows, r * rows + mast)
        agg[some, :] = dot(adj[some, :], table[...]).astype(BF16)

    for h in (0, 1):
        cols = slice(h * half, (h + 1) * half)
        part = dot(table[:mast, :], selfw[:, cols])
        for r in range(rel):
            part += dot(agg[r * rows : r * rows + mast, :], relw[r, :, cols])
        own[2 * h] = part[:, :slab]
        own[2 * h + 1] = part[:, slab:]

    def transposed(values):
        turned = values.astype(F32).T.reshape(nx * ny, 2, piece, values.shape[0])
        return [turned[:, core].reshape(half, values.shape[0]).astype(BF16) for core in (0, 1)]

    for r in range(rel):
        for core, values in enumerate(transposed(agg[r * rows : (r + 1) * rows, :])):
            agg_t[r, core] = values
    for core, values in enumerate(transposed(table[:mast, :])):
        agg_t[rel, core, :, :mast] = values

    counted(adj_t, source[...], target[...])

    def gpull(b, k):
        at = gtab.at[b // 2, mirror_rows(), pl.ds((b % 2) * slab, slab)]
        return remote(gsend.at[b, zp(k)], at, s_gpull.at[b, k], r_gpull.at[b, k], dom=zp(k))

    for b in range(4):
        for k in ring:
            push(b, k).wait_recv()
        cols = slice(b * slab, (b + 1) * slab)
        part_cols = slice((b % 2) * slab, (b % 2 + 1) * slab)
        value = own[b] + dot(place[...], qrecv[b].reshape(mirrors, slab))
        gate = 1.0 / (1.0 + jnp.exp(-value))
        grad = (cotan[:, cols].astype(F32) * gate * (1.0 + value * (1.0 - gate))).astype(BF16)
        gsend[b] = dot(pick[...], grad).astype(BF16).reshape(nz, cap, slab)
        for k in ring:
            send(gpull(b, k))
        gtab[b // 2, :mast, part_cols] = grad
        gtab[b // 2, mirror_rows(), part_cols] = gsend[b, z]
        act_ref[0, :, cols] = (value * gate).astype(BF16)

    def to_core(h, r):
        return remote(csend.at[h, r], crecv.at[h, r], s_core.at[h, r], r_core.at[h, r], grp_2=1 - c)

    def local(h, r):
        seen = mast if r == rel else rows
        csend[h, r] = dot(agg_t[r, 1 - c, :, :seen], gtab[h, :seen, :]).astype(BF16)
        send(to_core(h, r))
        lg[h, r] = dot(agg_t[r, c, :, :seen], gtab[h, :seen, :])

    mrow = half // nx

    def block(owner):
        return pl.ds(pl.multiple_of(lax.rem(owner, nx) * mrow, mrow), mrow)

    def along_x(h, r, k):
        return remote(
            xs.at[h, r, block(x + k), :], xr.at[h, r, k], s_x.at[h, r, k], r_x.at[h, r, k], grp_0=lax.rem(x + k, nx)
        )

    def over_x(h, r):
        to_core(h, r).wait_recv()
        lg[h, r] = lg[h, r] + crecv[h, r].astype(F32)
        xs[h, r] = lg[h, r].astype(BF16)
        for k in nearest_last(nx):
            send(along_x(h, r, k))

    def along_y(h, r, k):
        to = lax.rem(y + k, ny)
        return remote(ysend.at[h, r, to], yr.at[h, r, k], s_y.at[h, r, k], r_y.at[h, r, k], grp_1=to)

    def over_y(h, r):
        total = lg[h, r, block(x), :]
        for k in range(1, nx):
            along_x(h, r, k).wait_recv()
            total += xr[h, r, k].astype(F32)
        ymine[h, r] = total
        ysend[h, r] = ymine[h, r].reshape(ny, piece, half).astype(BF16)
        for k in yring:
            send(along_y(h, r, k))

    parts = 2 * (rel + 1)
    held = -(-parts // GROUP)
    owners = nz // GROUP

    def piece_of(h, r):
        return h if r == rel else 2 + h * rel + r

    def along_z(q, j):
        owner = q % GROUP + j * GROUP
        k = lax.rem(owner - z + 2 * nz, nz)
        return remote(zsend.at[q], zrecv.at[q // GROUP, k], s_z.at[q, j], r_z.at[q // GROUP, k], dom=owner)

    def over_z(h, r):
        q = piece_of(h, r)
        total = ymine[h, r, pl.ds(pl.multiple_of(y * piece, piece), piece), :]
        for k in yring:
            along_y(h, r, k).wait_recv()
            total += yr[h, r, k].astype(F32)
        zmine[q] = total
        zsend[q] = total.astype(BF16)
        for j in range(owners):
            @pl.when(z != q % GROUP + j * GROUP)
            def _():
                along_z(q, j).start()

    def shared(i, k):
        q = lax.rem(z, GROUP) + i * GROUP
        return remote(zown.at[i], wrecv.at[q], s_w.at[i, k], r_w.at[q], dom=zp(k))

    near = (2, nz - 1, 1)

    def total_z(i):
        q = lax.rem(z, GROUP) + i * GROUP

        @pl.when(q < parts)
        def _():
            total = zmine[q]
            for k in range(1, nz):
                remote(zsend.at[0], zrecv.at[i, k], s_z.at[0, 0], r_z.at[i, k], dom=zp(1)).wait_recv()
                total += zrecv[i, k].astype(F32)
            zown[i] = total
            for k in near:
                shared(i, k).start()
            wrecv[q] = total

    def units(h):
        return [(h, r) for r in range(rel)]

    first = [(0, rel), (1, rel)]
    for u in first:
        local(*u)
    for u in first:
        over_x(*u)

    for k in ring:
        gpull(0, k).wait_recv()
        gpull(1, k).wait_recv()
    for u in units(0):
        local(*u)
    for u in units(0):
        over_x(*u)
    for u in first:
        over_y(*u)

    for k in ring:
        gpull(2, k).wait_recv()
        gpull(3, k).wait_recv()
    for u in units(1):
        local(*u)
    for u in units(1):
        over_x(*u)

    for h in (0, 1):
        back[:, h * half : (h + 1) * half] = dot(adj_t[...], gtab[h]).astype(BF16)
    part = dot_nt(back[mast:rows, :], relw[0])
    for r in range(1, rel):
        part += dot_nt(back[r * rows + mast : (r + 1) * rows, :], relw[r])
    bsend[...] = part.astype(BF16).reshape(nz, cap, width)
    brecv[z] = bsend[z]

    def bpush(k):
        return remote(bsend.at[zp(k)], brecv.at[z], s_back.at[k], r_back.at[k], dom=zp(k))

    for k in ring:
        send(bpush(k))

    for u in units(0):
        over_y(*u)
    for u in first:
        over_z(*u)

    part = dot_nt(gtab[0, :mast, :], selfw[:, :half]) + dot_nt(gtab[1, :mast, :], selfw[:, half:])
    for r in range(rel):
        part += dot_nt(back[r * rows : r * rows + mast, :], relw[r])
    bown[...] = part

    for u in units(1):
        over_y(*u)
    for u in units(0):
        over_z(*u)
    for u in units(1):
        over_z(*u)
    total_z(0)

    for k in ring:
        bpush(k).wait_recv()
    ingrad_ref[0] = (bown[...] + dot(place[...], brecv[...].reshape(mirrors, width))).astype(BF16)

    for i in range(1, held):
        total_z(i)

    for h in (0, 1):
        for r in range(rel + 1):
            q = piece_of(h, r)

            @pl.when(lax.rem(z, GROUP) != q % GROUP)
            def _():
                remote(zown.at[0], wrecv.at[q], s_w.at[0, 1], r_w.at[q], dom=zp(1)).wait_recv()

            wgrad_ref[r, :, h * half : (h + 1) * half] = wrecv[q]

    for copy in sent:
        copy.wait_send()
    for q in range(parts):
        for j in range(owners):
            @pl.when(z != q % GROUP + j * GROUP)
            def _():
                along_z(q, j).wait_send()
    for i in range(held):
        @pl.when(lax.rem(z, GROUP) + i * GROUP < parts)
        def _():
            for k in near:
                shared(i, k).wait_send()


def handed_on(*refs):
    half = len(refs) // 2
    for a, b in zip(refs[:half], refs[half:]):
        b[...] = a[...]


def per_device(
    master_rows, cotangent, relation_weight, self_weight, edge_source, edge_target, edge_relation, send_rows,
    send_counts,
):
    nz = lax.axis_size("dom")
    ny = lax.axis_size("grp_1")
    rel, width = relation_weight.shape[:2]
    mast = master_rows.shape[1]
    mirrors = send_rows.shape[1]
    cap = mirrors // nz
    rows = mast + mirrors
    edges = edge_source.shape[1]
    half = width // 2
    slab = width // 4
    nx = NX
    mrow = half // nx
    piece = width // (nx * ny * 2)
    parts = 2 * (rel + 1)
    held = -(-parts // GROUP)
    vmem = pl.BlockSpec(memory_space=pltpu.VMEM)
    hbm = pl.BlockSpec(memory_space=pl.ANY)
    dma = pltpu.SemaphoreType.DMA
    scratch = [
        pltpu.SMEM((1, nz), jnp.int32),
        pltpu.VMEM((mast, width), BF16),
        pltpu.VMEM((1, edges), jnp.int32),
        pltpu.VMEM((1, edges), jnp.int32),
        pltpu.VMEM((1, edges), jnp.int32),
        pltpu.VMEM((1, mirrors), jnp.int32),
        pltpu.VMEM((rel, width, width), BF16),
        pltpu.VMEM((width, width), BF16),
        pltpu.VMEM((rows, edges), BF16),
        pltpu.VMEM((rel * rows, rows), BF16),
        pltpu.VMEM((rel * rows, rows), BF16),
        pltpu.VMEM((mast, mirrors), BF16),
        pltpu.VMEM((mirrors, mast), BF16),
        pltpu.VMEM((rows, width), BF16),
        pltpu.VMEM((rel * rows, width), BF16),
        pltpu.VMEM((rel + 1, 2, half, rows), BF16),
        pltpu.VMEM((nz, cap, width), BF16),
        pltpu.VMEM((4, nz, cap, slab), BF16),
        pltpu.VMEM((4, nz, cap, slab), BF16),
        pltpu.VMEM((4, mast, slab), F32),
        pltpu.VMEM((4, nz, cap, slab), BF16),
        pltpu.VMEM((2, rows, half), BF16),
        pltpu.VMEM((rel * rows, width), BF16),
        pltpu.VMEM((mast, width), F32),
        pltpu.VMEM((nz, cap, width), BF16),
        pltpu.VMEM((nz, cap, width), BF16),
        pltpu.VMEM((2, rel + 1, half, half), BF16),
        pltpu.VMEM((2, rel + 1, half, half), BF16),
        pltpu.VMEM((2, rel + 1, half, half), F32),
        pltpu.VMEM((2, rel + 1, half, half), BF16),
        pltpu.VMEM((2, rel + 1, nx, mrow, half), BF16),
        pltpu.VMEM((2, rel + 1, ny, piece, half), BF16),
        pltpu.VMEM((2, rel + 1, mrow, half), F32),
        pltpu.VMEM((2, rel + 1, ny, piece, half), BF16),
        pltpu.VMEM((parts, piece, half), F32),
        pltpu.VMEM((parts, piece, half), BF16),
        pltpu.VMEM((held, nz, piece, half), BF16),
        pltpu.VMEM((held, piece, half), F32),
        pltpu.VMEM((parts, piece, half), F32),
        dma((9,)),
        dma((nz,)), dma((nz,)),
        dma((4, nz)), dma((4, nz)),
        dma((4, nz)), dma((4, nz)),
        dma((nz,)), dma((nz,)),
        dma((2, rel + 1)), dma((2, rel + 1)),
        dma((2, rel + 1, nx)), dma((2, rel + 1, nx)),
        dma((2, rel + 1, ny)), dma((2, rel + 1, ny)),
        dma((parts, nz // GROUP)), dma((held, nz)),
        dma((held, nz)), dma((parts,)),
    ]
    out_shape = (
        jax.ShapeDtypeStruct((1, mast, width), BF16),
        jax.ShapeDtypeStruct((1, mast, width), BF16),
        jax.ShapeDtypeStruct((rel + 1, piece, width), F32),
    )
    results = pl.pallas_call(
        functools.partial(kernel, nz, ny, cap),
        out_shape=tuple(pltpu.VMEM(o.shape, o.dtype) for o in out_shape),
        in_specs=[hbm] * 9,
        out_specs=(vmem, vmem, vmem),
        scratch_shapes=scratch,
        compiler_params=pltpu.CompilerParams(
            collective_id=0, has_side_effects=True, vmem_limit_bytes=56 * 1024 * 1024
        ),
        name="graph_conv_step",
    )(
        send_counts, master_rows, cotangent, edge_source, edge_target, edge_relation, send_rows, relation_weight,
        self_weight,
    )
    return pl.pallas_call(
        handed_on,
        out_shape=out_shape,
        in_specs=[vmem] * 3,
        out_specs=(vmem, vmem, vmem),
        compiler_params=pltpu.CompilerParams(vmem_limit_bytes=4 * 1024 * 1024),
        name="handed_on",
    )(*results)


def solution(mesh):
    devices = mesh.devices.shape[1]
    finer = Mesh(
        mesh.devices.reshape(mesh.shape["dom"], NX, devices // (2 * NX), 2), ("dom", "grp_0", "grp_1", "grp_2")
    )
    in_specs = (
        P(GRP, "dom", None),
        P(GRP, "dom", None),
        P(),
        P(),
        P(GRP, "dom"),
        P(GRP, "dom"),
        P(GRP, "dom"),
        P(GRP, "dom"),
        P(GRP, "dom"),
    )
    out_specs = (P(GRP, "dom", None), P(GRP, "dom", None), P(None, GRP, None))
    return jax.shard_map(per_device, mesh=finer, in_specs=in_specs, out_specs=out_specs, check_vma=False)
```

```python
import functools

import jax
import jax.numpy as jnp
from jax import lax
from jax.experimental import pallas as pl
from jax.experimental.pallas import tpu as pltpu
from jax.sharding import Mesh
from jax.sharding import PartitionSpec as P

GRP = ("grp_0", "grp_1", "grp_2")
MESH = pl.DeviceIdType.MESH
NX = 4
GROUP = 4
F32 = jnp.float32
BF16 = jnp.bfloat16


def dot(a, b):
    return jnp.dot(a, b, preferred_element_type=F32)


def dot_nt(a, b):
    return lax.dot_general(a, b, (((1,), (1,)), ((), ())), preferred_element_type=F32)


def nearest_last(n):
    return sorted(range(1, n), key=lambda k: (-min(k, n - k), k))


def kernel(
    nz, ny, cap,
    counts_hbm, masters_hbm, cotan_hbm, source_hbm, target_hbm, relation_hbm, slots_hbm, relw_hbm, selfw_hbm,
    act_ref, ingrad_ref, wgrad_ref,
    counts, cotan, source, target, relation, slots, relw, selfw, one_hot, adj, adj_t, place, pick, table, agg, agg_t,
    psend, qsend, qrecv, own, gsend, gtab, back, bown, bsend, brecv, self_t, pagg, pself, pgt, lg, xs, xr, ysend, ymine, yr,
    fs, fyr, fmine, fxs, fxr, zmine, zsend, zrecv, zown, wrecv,
    in_sem, s_pull, r_pull, s_push, r_push, s_gpull, r_gpull, s_back, r_back, s_core, r_core, s_x, r_x, s_y, r_y,
    s_fy, r_fy, s_fx, r_fx, s_z, r_z, s_w, r_w,
):
    z = lax.axis_index("dom")
    x = lax.axis_index("grp_0")
    y = lax.axis_index("grp_1")
    c = lax.axis_index("grp_2")
    nx = NX
    rel = relw.shape[0]
    width = relw.shape[1]
    half = width // 2
    slab = width // 4
    mast = cotan.shape[0]
    rows = table.shape[0]
    mirrors = rows - mast
    piece = width // (nx * ny * 2)
    ring = nearest_last(nz)
    yring = nearest_last(ny)
    sent = []

    def zp(k):
        return lax.rem(z + k, nz)

    def send(copy):
        copy.start()
        sent.append(copy)

    def remote(src, dst, send_sem, recv_sem, **device):
        return pltpu.make_async_remote_copy(
            src_ref=src, dst_ref=dst, send_sem=send_sem, recv_sem=recv_sem, device_id=device, device_id_type=MESH
        )

    barrier = pltpu.get_barrier_semaphore()
    met = [{"dom": zp(k)} for k in ring] + [{"grp_1": lax.rem(y + k, ny)} for k in yring]
    met += [{"grp_0": lax.rem(x + k, nx)} for k in range(1, nx)] + [{"grp_2": 1 - c}]
    for device in met:
        pl.semaphore_signal(barrier, inc=1, device_id=device, device_id_type=MESH)

    brought = (
        (counts_hbm, counts), (slots_hbm, slots), (masters_hbm.at[0], table.at[:mast]), (target_hbm, target),
        (source_hbm, source), (relation_hbm, relation), (relw_hbm, relw), (selfw_hbm, selfw),
        (cotan_hbm.at[0], cotan),
    )
    inputs = [pltpu.make_async_copy(a, b, in_sem.at[i]) for i, (a, b) in enumerate(brought)]
    for copy in inputs:
        copy.start()
    for copy in inputs[:2]:
        copy.wait()

    lane = lax.broadcasted_iota(jnp.int32, (1, mirrors), 1)
    limit = jnp.zeros((1, mirrors), jnp.int32)
    for p in range(nz):
        limit = jnp.where((lane >= p * cap) & (lane < (p + 1) * cap), counts[0, p] + p * cap, limit)
    named = jnp.where(lane < limit, slots[...], -1)
    row = lax.broadcasted_iota(jnp.int32, (mast, mirrors), 0)
    placement = jnp.where(row == named, 1.0, 0.0)
    place[...] = placement.astype(BF16)
    pick[...] = placement.T.astype(BF16)

    inputs[2].wait()
    psend[...] = dot(pick[...], table[:mast, :]).astype(BF16).reshape(nz, cap, width)

    def mirror_rows():
        return pl.ds(pl.multiple_of(mast + z * cap, cap), cap)

    def pull(k):
        return remote(psend.at[zp(k)], table.at[mirror_rows(), :], s_pull.at[k], r_pull.at[k], dom=zp(k))

    pl.semaphore_wait(barrier, len(met))
    for k in ring:
        send(pull(k))
    table[mirror_rows(), :] = psend[z]

    for copy in inputs[3:6]:
        copy.wait()
    row = lax.broadcasted_iota(jnp.int32, (rows, source.shape[1]), 0)

    def counted(dst, first, second):
        one_hot[...] = jnp.where(row == second, 1.0, 0.0).astype(BF16)

        @pl.loop(0, rel)
        def _(r):
            mine = jnp.where(relation[...] == r, first, -1)
            hot = jnp.where(row == mine, 1.0, 0.0).astype(BF16)
            dst[pl.ds(pl.multiple_of(r * rows, rows), rows), :] = dot_nt(hot, one_hot[...]).astype(BF16)

    counted(adj, target[...], source[...])
    for copy in inputs[6:]:
        copy.wait()

    for k in ring:
        pull(k).wait_recv()
    for r in range(rel):
        some = slice(r * rows + mast, (r + 1) * rows)
        agg[some, :] = dot(adj[some, :], table[...]).astype(BF16)

    def push(b, k):
        return remote(qsend.at[b, zp(k)], qrecv.at[b, z], s_push.at[b, k], r_push.at[b, k], dom=zp(k))

    for h in (0, 1):
        cols = slice(h * half, (h + 1) * half)
        part = dot(agg[mast:rows, :], relw[0, :, cols])
        for r in range(1, rel):
            part += dot(agg[r * rows + mast : (r + 1) * rows, :], relw[r, :, cols])
        for b in (2 * h, 2 * h + 1):
            qsend[b] = part[:, (b % 2) * slab : (b % 2 + 1) * slab].astype(BF16).reshape(nz, cap, slab)
            qrecv[b, z] = qsend[b, z]
            for k in ring:
                send(push(b, k))

    for r in range(rel):
        some = slice(r * rows, r * rows + mast)
        agg[some, :] = dot(adj[some, :], table[...]).astype(BF16)

    for h in (0, 1):
        cols = slice(h * half, (h + 1) * half)
        part = dot(table[:mast, :], selfw[:, cols])
        for r in range(rel):
            part += dot(agg[r * rows : r * rows + mast, :], relw[r, :, cols])
        own[2 * h] = part[:, :slab]
        own[2 * h + 1] = part[:, slab:]

    def transposed(values):
        turned = values.astype(F32).T.reshape(nx * ny, 2, piece, values.shape[0])
        return [turned[:, core].reshape(half, values.shape[0]).astype(BF16) for core in (0, 1)]

    for r in range(rel):
        for core, values in enumerate(transposed(agg[r * rows : (r + 1) * rows, :])):
            agg_t[r, core] = values
    for core, values in enumerate(transposed(table[:mast, :])):
        self_t[core] = values

    def to_core(src, dst, n):
        return remote(src, dst, s_core.at[n], r_core.at[n], grp_2=1 - c)

    give_agg = to_core(agg_t.at[:, 1 - c], pagg, 0)
    give_self = to_core(self_t.at[1 - c], pself, 1)
    send(give_agg)
    send(give_self)

    def give_masters(h):
        return to_core(gtab.at[h, :mast, :], pgt.at[h, :mast, :], 2 + h)

    def give_mirrors(h):
        return to_core(gtab.at[h, mast:, :], pgt.at[h, mast:, :], 4 + h)

    counted(adj_t, source[...], target[...])

    def gpull(b, k):
        at = gtab.at[b // 2, mirror_rows(), pl.ds((b % 2) * slab, slab)]
        return remote(gsend.at[b, zp(k)], at, s_gpull.at[b, k], r_gpull.at[b, k], dom=zp(k))

    for b in range(4):
        for k in ring:
            push(b, k).wait_recv()
        cols = slice(b * slab, (b + 1) * slab)
        part_cols = slice((b % 2) * slab, (b % 2 + 1) * slab)
        value = own[b] + dot(place[...], qrecv[b].reshape(mirrors, slab))
        gate = 1.0 / (1.0 + jnp.exp(-value))
        grad = (cotan[:, cols].astype(F32) * gate * (1.0 + value * (1.0 - gate))).astype(BF16)
        gsend[b] = dot(pick[...], grad).astype(BF16).reshape(nz, cap, slab)
        for k in ring:
            send(gpull(b, k))
        gtab[b // 2, :mast, part_cols] = grad
        gtab[b // 2, mirror_rows(), part_cols] = gsend[b, z]
        act_ref[0, :, cols] = (value * gate).astype(BF16)
        if b % 2:
            send(give_masters(b // 2))

    swapped = rel - 1

    mrow = half // nx

    def block(owner):
        return pl.ds(pl.multiple_of(lax.rem(owner, nx) * mrow, mrow), mrow)

    def along_x(h, r, k):
        return remote(
            xs.at[h, r, block(x + k), :], xr.at[h, r, k], s_x.at[h, r, k], r_x.at[h, r, k], grp_0=lax.rem(x + k, nx)
        )

    def over_x(h, r):
        xs[h, r] = lg[h, r].astype(BF16)
        for k in nearest_last(nx):
            send(along_x(h, r, k))

    def along_y_first(h, k):
        to = lax.rem(y + k, ny)
        return remote(fs.at[h, :, to], fyr.at[h, k], s_fy.at[h, k], r_fy.at[h, k], grp_1=to)

    def over_y_first(h):
        fs[h] = lg[h, swapped].reshape(nx, ny, piece, half).astype(BF16)
        for k in yring:
            send(along_y_first(h, k))

    def along_x_last(h, k):
        to = lax.rem(x + k, nx)
        return remote(fxs.at[h, to], fxr.at[h, k], s_fx.at[h, k], r_fx.at[h, k], grp_0=to)

    def over_x_last(h):
        for k in yring:
            along_y_first(h, k).wait_recv()
        for owner in range(nx):
            total = lg[h, swapped, pl.ds(pl.multiple_of((owner * ny + y) * piece, piece), piece), :]
            for k in yring:
                total += fyr[h, k, owner].astype(F32)
            fmine[h, owner] = total
            fxs[h, owner] = total.astype(BF16)
        for k in nearest_last(nx):
            send(along_x_last(h, k))

    def along_y(h, r, k):
        to = lax.rem(y + k, ny)
        return remote(ysend.at[h, r, to], yr.at[h, r, k], s_y.at[h, r, k], r_y.at[h, r, k], grp_1=to)

    def over_y(h, r):
        total = lg[h, r, block(x), :]
        for k in range(1, nx):
            along_x(h, r, k).wait_recv()
            total += xr[h, r, k].astype(F32)
        ymine[h, r] = total
        ysend[h, r] = ymine[h, r].reshape(ny, piece, half).astype(BF16)
        for k in yring:
            send(along_y(h, r, k))

    parts = 2 * (rel + 1)
    held = -(-parts // GROUP)
    owners = nz // GROUP

    def piece_of(h, r):
        return h if r == rel else 2 + h * rel + r

    def along_z(q, j):
        owner = q % GROUP + j * GROUP
        k = lax.rem(owner - z + 2 * nz, nz)
        return remote(zsend.at[q], zrecv.at[q // GROUP, k], s_z.at[q, j], r_z.at[q // GROUP, k], dom=owner)

    def over_z(h, r):
        q = piece_of(h, r)
        if r == swapped:
            total = fmine[h, x]
            for k in range(1, nx):
                along_x_last(h, k).wait_recv()
                total += fxr[h, k].astype(F32)
        else:
            total = ymine[h, r, pl.ds(pl.multiple_of(y * piece, piece), piece), :]
            for k in yring:
                along_y(h, r, k).wait_recv()
                total += yr[h, r, k].astype(F32)
        zmine[q] = total
        zsend[q] = total.astype(BF16)
        for j in range(owners):
            @pl.when(z != q % GROUP + j * GROUP)
            def _():
                along_z(q, j).start()

    def shared(i, k):
        q = lax.rem(z, GROUP) + i * GROUP
        return remote(zown.at[i], wrecv.at[q], s_w.at[i, k], r_w.at[q], dom=zp(k))

    near = (2, nz - 1, 1)

    def total_z(i):
        q = lax.rem(z, GROUP) + i * GROUP

        @pl.when(q < parts)
        def _():
            total = zmine[q]
            for k in range(1, nz):
                remote(zsend.at[0], zrecv.at[i, k], s_z.at[0, 0], r_z.at[i, k], dom=zp(1)).wait_recv()
                total += zrecv[i, k].astype(F32)
            zown[i] = total
            for k in near:
                shared(i, k).start()
            wrecv[q] = total

    def units(h):
        return [(h, r) for r in range(rel) if r != swapped]

    first = [(0, rel), (1, rel)]
    give_agg.wait_recv()
    give_self.wait_recv()
    for h in (0, 1):
        give_masters(h).wait_recv()
        lg[h, rel] = dot(self_t[c], gtab[h, :mast, :]) + dot(pself[...], pgt[h, :mast, :])
        over_x(h, rel)

    for h in (0, 1):
        for k in ring:
            gpull(2 * h, k).wait_recv()
            gpull(2 * h + 1, k).wait_recv()
        send(give_mirrors(h))
        order = [swapped] + list(range(swapped))
        for r in order:
            lg[h, r] = dot(agg_t[r, c], gtab[h])
        give_mirrors(h).wait_recv()
        for r in order:
            lg[h, r] = lg[h, r] + dot(pagg[r], pgt[h])
            if r == swapped:
                over_y_first(h)
            else:
                over_x(h, r)
        if h == 0:
            for u in first:
                over_y(*u)

    for h in (0, 1):
        back[:, h * half : (h + 1) * half] = dot(adj_t[...], gtab[h]).astype(BF16)
    part = dot_nt(back[mast:rows, :], relw[0])
    for r in range(1, rel):
        part += dot_nt(back[r * rows + mast : (r + 1) * rows, :], relw[r])
    bsend[...] = part.astype(BF16).reshape(nz, cap, width)
    brecv[z] = bsend[z]

    def bpush(k):
        return remote(bsend.at[zp(k)], brecv.at[z], s_back.at[k], r_back.at[k], dom=zp(k))

    for k in ring:
        send(bpush(k))

    for u in units(0):
        over_y(*u)
    for u in first:
        over_z(*u)
    over_x_last(0)

    part = dot_nt(gtab[0, :mast, :], selfw[:, :half]) + dot_nt(gtab[1, :mast, :], selfw[:, half:])
    for r in range(rel):
        part += dot_nt(back[r * rows : r * rows + mast, :], relw[r])
    bown[...] = part

    for u in units(1):
        over_y(*u)
    for u in units(0):
        over_z(*u)
    over_z(0, swapped)
    over_x_last(1)
    for u in units(1):
        over_z(*u)
    over_z(1, swapped)
    total_z(0)

    for k in ring:
        bpush(k).wait_recv()
    ingrad_ref[0] = (bown[...] + dot(place[...], brecv[...].reshape(mirrors, width))).astype(BF16)

    for i in range(1, held):
        total_z(i)

    for h in (0, 1):
        for r in range(rel + 1):
            q = piece_of(h, r)

            @pl.when(lax.rem(z, GROUP) != q % GROUP)
            def _():
                remote(zown.at[0], wrecv.at[q], s_w.at[0, 1], r_w.at[q], dom=zp(1)).wait_recv()

            wgrad_ref[r, :, h * half : (h + 1) * half] = wrecv[q]

    for copy in sent:
        copy.wait_send()
    for q in range(parts):
        for j in range(owners):
            @pl.when(z != q % GROUP + j * GROUP)
            def _():
                along_z(q, j).wait_send()
    for i in range(held):
        @pl.when(lax.rem(z, GROUP) + i * GROUP < parts)
        def _():
            for k in near:
                shared(i, k).wait_send()


def handed_on(*refs):
    half = len(refs) // 2
    for a, b in zip(refs[:half], refs[half:]):
        b[...] = a[...]


def per_device(
    master_rows, cotangent, relation_weight, self_weight, edge_source, edge_target, edge_relation, send_rows,
    send_counts,
):
    nz = lax.axis_size("dom")
    ny = lax.axis_size("grp_1")
    rel, width = relation_weight.shape[:2]
    mast = master_rows.shape[1]
    mirrors = send_rows.shape[1]
    cap = mirrors // nz
    rows = mast + mirrors
    edges = edge_source.shape[1]
    half = width // 2
    slab = width // 4
    nx = NX
    mrow = half // nx
    piece = width // (nx * ny * 2)
    parts = 2 * (rel + 1)
    held = -(-parts // GROUP)
    vmem = pl.BlockSpec(memory_space=pltpu.VMEM)
    hbm = pl.BlockSpec(memory_space=pl.ANY)
    dma = pltpu.SemaphoreType.DMA
    scratch = [
        pltpu.SMEM((1, nz), jnp.int32),
        pltpu.VMEM((mast, width), BF16),
        pltpu.VMEM((1, edges), jnp.int32),
        pltpu.VMEM((1, edges), jnp.int32),
        pltpu.VMEM((1, edges), jnp.int32),
        pltpu.VMEM((1, mirrors), jnp.int32),
        pltpu.VMEM((rel, width, width), BF16),
        pltpu.VMEM((width, width), BF16),
        pltpu.VMEM((rows, edges), BF16),
        pltpu.VMEM((rel * rows, rows), BF16),
        pltpu.VMEM((rel * rows, rows), BF16),
        pltpu.VMEM((mast, mirrors), BF16),
        pltpu.VMEM((mirrors, mast), BF16),
        pltpu.VMEM((rows, width), BF16),
        pltpu.VMEM((rel * rows, width), BF16),
        pltpu.VMEM((rel, 2, half, rows), BF16),
        pltpu.VMEM((nz, cap, width), BF16),
        pltpu.VMEM((4, nz, cap, slab), BF16),
        pltpu.VMEM((4, nz, cap, slab), BF16),
        pltpu.VMEM((4, mast, slab), F32),
        pltpu.VMEM((4, nz, cap, slab), BF16),
        pltpu.VMEM((2, rows, half), BF16),
        pltpu.VMEM((rel * rows, width), BF16),
        pltpu.VMEM((mast, width), F32),
        pltpu.VMEM((nz, cap, width), BF16),
        pltpu.VMEM((nz, cap, width), BF16),
        pltpu.VMEM((2, half, mast), BF16),
        pltpu.VMEM((rel, half, rows), BF16),
        pltpu.VMEM((half, mast), BF16),
        pltpu.VMEM((2, rows, half), BF16),
        pltpu.VMEM((2, rel + 1, half, half), F32),
        pltpu.VMEM((2, rel + 1, half, half), BF16),
        pltpu.VMEM((2, rel + 1, nx, mrow, half), BF16),
        pltpu.VMEM((2, rel + 1, ny, piece, half), BF16),
        pltpu.VMEM((2, rel + 1, mrow, half), F32),
        pltpu.VMEM((2, rel + 1, ny, piece, half), BF16),
        pltpu.VMEM((2, nx, ny, piece, half), BF16),
        pltpu.VMEM((2, ny, nx, piece, half), BF16),
        pltpu.VMEM((2, nx, piece, half), F32),
        pltpu.VMEM((2, nx, piece, half), BF16),
        pltpu.VMEM((2, nx, piece, half), BF16),
        pltpu.VMEM((parts, piece, half), F32),
        pltpu.VMEM((parts, piece, half), BF16),
        pltpu.VMEM((held, nz, piece, half), BF16),
        pltpu.VMEM((held, piece, half), F32),
        pltpu.VMEM((parts, piece, half), F32),
        dma((9,)),
        dma((nz,)), dma((nz,)),
        dma((4, nz)), dma((4, nz)),
        dma((4, nz)), dma((4, nz)),
        dma((nz,)), dma((nz,)),
        dma((6,)), dma((6,)),
        dma((2, rel + 1, nx)), dma((2, rel + 1, nx)),
        dma((2, rel + 1, ny)), dma((2, rel + 1, ny)),
        dma((2, ny)), dma((2, ny)),
        dma((2, nx)), dma((2, nx)),
        dma((parts, nz // GROUP)), dma((held, nz)),
        dma((held, nz)), dma((parts,)),
    ]
    out_shape = (
        jax.ShapeDtypeStruct((1, mast, width), BF16),
        jax.ShapeDtypeStruct((1, mast, width), BF16),
        jax.ShapeDtypeStruct((rel + 1, piece, width), F32),
    )
    results = pl.pallas_call(
        functools.partial(kernel, nz, ny, cap),
        out_shape=tuple(pltpu.VMEM(o.shape, o.dtype) for o in out_shape),
        in_specs=[hbm] * 9,
        out_specs=(vmem, vmem, vmem),
        scratch_shapes=scratch,
        compiler_params=pltpu.CompilerParams(
            collective_id=0, has_side_effects=True, vmem_limit_bytes=56 * 1024 * 1024
        ),
        name="graph_conv_step",
    )(
        send_counts, master_rows, cotangent, edge_source, edge_target, edge_relation, send_rows, relation_weight,
        self_weight,
    )
    return pl.pallas_call(
        handed_on,
        out_shape=out_shape,
        in_specs=[vmem] * 3,
        out_specs=(vmem, vmem, vmem),
        compiler_params=pltpu.CompilerParams(vmem_limit_bytes=4 * 1024 * 1024),
        name="handed_on",
    )(*results)


def solution(mesh):
    devices = mesh.devices.shape[1]
    finer = Mesh(
        mesh.devices.reshape(mesh.shape["dom"], NX, devices // (2 * NX), 2), ("dom", "grp_0", "grp_1", "grp_2")
    )
    in_specs = (
        P(GRP, "dom", None),
        P(GRP, "dom", None),
        P(),
        P(),
        P(GRP, "dom"),
        P(GRP, "dom"),
        P(GRP, "dom"),
        P(GRP, "dom"),
        P(GRP, "dom"),
    )
    out_specs = (P(GRP, "dom", None), P(GRP, "dom", None), P(None, GRP, None))
    return jax.shard_map(per_device, mesh=finer, in_specs=in_specs, out_specs=out_specs, check_vma=False)
```

```python
import functools

import jax
import jax.numpy as jnp
from jax import lax
from jax.experimental import pallas as pl
from jax.experimental.pallas import tpu as pltpu
from jax.sharding import Mesh
from jax.sharding import PartitionSpec as P

GRP = ("grp_0", "grp_1", "grp_2")
MESH = pl.DeviceIdType.MESH
NX = 4
GROUP = 4
F32 = jnp.float32
BF16 = jnp.bfloat16


def dot(a, b):
    return jnp.dot(a, b, preferred_element_type=F32)


def dot_nt(a, b):
    return lax.dot_general(a, b, (((1,), (1,)), ((), ())), preferred_element_type=F32)


def nearest_last(n):
    return sorted(range(1, n), key=lambda k: (-min(k, n - k), k))


def kernel(
    nz, ny, cap,
    counts_hbm, masters_hbm, cotan_hbm, source_hbm, target_hbm, relation_hbm, slots_hbm, relw_hbm, selfw_hbm,
    act_ref, ingrad_ref, wgrad_ref,
    counts, cotan, source, target, relation, slots, relw, selfw, one_hot, adj, adj_t, place, pick, table, agg, agg_t,
    psend, qsend, qrecv, own, gsend, gtab, back, bown, bsend, brecv, self_t, pagg, pself, pgt, s_arrays, w_arrays,
    flg, fs, fyr, fmine, fxs, fxr, zmine, zsend, zrecv, zown, wrecv,
    in_sem, s_pull, r_pull, s_push, r_push, s_gpull, r_gpull, s_back, r_back, s_core, r_core,
    s_fy, r_fy, s_fx, r_fx, s_z, r_z, s_w, r_w,
):
    z = lax.axis_index("dom")
    x = lax.axis_index("grp_0")
    y = lax.axis_index("grp_1")
    c = lax.axis_index("grp_2")
    nx = NX
    rel = relw.shape[0]
    width = relw.shape[1]
    half = width // 2
    slab = width // 4
    mast = cotan.shape[0]
    rows = table.shape[0]
    mirrors = rows - mast
    piece = width // (nx * ny * 2)
    ring = nearest_last(nz)
    yring = nearest_last(ny)
    sent = []

    def zp(k):
        return lax.rem(z + k, nz)

    def send(copy):
        copy.start()
        sent.append(copy)

    def remote(src, dst, send_sem, recv_sem, **device):
        return pltpu.make_async_remote_copy(
            src_ref=src, dst_ref=dst, send_sem=send_sem, recv_sem=recv_sem, device_id=device, device_id_type=MESH
        )

    barrier = pltpu.get_barrier_semaphore()
    met = [{"dom": zp(k)} for k in ring] + [{"grp_1": lax.rem(y + k, ny)} for k in yring]
    met += [{"grp_0": lax.rem(x + k, nx)} for k in range(1, nx)] + [{"grp_2": 1 - c}]
    for device in met:
        pl.semaphore_signal(barrier, inc=1, device_id=device, device_id_type=MESH)

    brought = (
        (counts_hbm, counts), (slots_hbm, slots), (masters_hbm.at[0], table.at[:mast]), (target_hbm, target),
        (source_hbm, source), (relation_hbm, relation), (relw_hbm, relw), (selfw_hbm, selfw),
        (cotan_hbm.at[0], cotan),
    )
    inputs = [pltpu.make_async_copy(a, b, in_sem.at[i]) for i, (a, b) in enumerate(brought)]
    for copy in inputs:
        copy.start()
    for copy in inputs[:2]:
        copy.wait()

    lane = lax.broadcasted_iota(jnp.int32, (1, mirrors), 1)
    limit = jnp.zeros((1, mirrors), jnp.int32)
    for p in range(nz):
        limit = jnp.where((lane >= p * cap) & (lane < (p + 1) * cap), counts[0, p] + p * cap, limit)
    named = jnp.where(lane < limit, slots[...], -1)
    row = lax.broadcasted_iota(jnp.int32, (mast, mirrors), 0)
    placement = jnp.where(row == named, 1.0, 0.0)
    place[...] = placement.astype(BF16)
    pick[...] = placement.T.astype(BF16)

    inputs[2].wait()
    psend[...] = dot(pick[...], table[:mast, :]).astype(BF16).reshape(nz, cap, width)

    def mirror_rows():
        return pl.ds(pl.multiple_of(mast + z * cap, cap), cap)

    def pull(k):
        return remote(psend.at[zp(k)], table.at[mirror_rows(), :], s_pull.at[k], r_pull.at[k], dom=zp(k))

    pl.semaphore_wait(barrier, len(met))
    for k in ring:
        send(pull(k))
    table[mirror_rows(), :] = psend[z]

    for copy in inputs[3:6]:
        copy.wait()
    row = lax.broadcasted_iota(jnp.int32, (rows, source.shape[1]), 0)

    def counted(dst, first, second):
        one_hot[...] = jnp.where(row == second, 1.0, 0.0).astype(BF16)

        @pl.loop(0, rel)
        def _(r):
            mine = jnp.where(relation[...] == r, first, -1)
            hot = jnp.where(row == mine, 1.0, 0.0).astype(BF16)
            dst[pl.ds(pl.multiple_of(r * rows, rows), rows), :] = dot_nt(hot, one_hot[...]).astype(BF16)

    counted(adj, target[...], source[...])
    for copy in inputs[6:]:
        copy.wait()

    for k in ring:
        pull(k).wait_recv()
    for r in range(rel):
        some = slice(r * rows + mast, (r + 1) * rows)
        agg[some, :] = dot(adj[some, :], table[...]).astype(BF16)

    def push(b, k):
        return remote(qsend.at[b, zp(k)], qrecv.at[b, z], s_push.at[b, k], r_push.at[b, k], dom=zp(k))

    for h in (0, 1):
        cols = slice(h * half, (h + 1) * half)
        part = dot(agg[mast:rows, :], relw[0, :, cols])
        for r in range(1, rel):
            part += dot(agg[r * rows + mast : (r + 1) * rows, :], relw[r, :, cols])
        for b in (2 * h, 2 * h + 1):
            qsend[b] = part[:, (b % 2) * slab : (b % 2 + 1) * slab].astype(BF16).reshape(nz, cap, slab)
            qrecv[b, z] = qsend[b, z]
            for k in ring:
                send(push(b, k))

    for r in range(rel):
        some = slice(r * rows, r * rows + mast)
        agg[some, :] = dot(adj[some, :], table[...]).astype(BF16)

    for h in (0, 1):
        cols = slice(h * half, (h + 1) * half)
        part = dot(table[:mast, :], selfw[:, cols])
        for r in range(rel):
            part += dot(agg[r * rows : r * rows + mast, :], relw[r, :, cols])
        own[2 * h] = part[:, :slab]
        own[2 * h + 1] = part[:, slab:]

    def transposed(values):
        turned = values.astype(F32).T.reshape(nx * ny, 2, piece, values.shape[0])
        return [turned[:, core].reshape(half, values.shape[0]).astype(BF16) for core in (0, 1)]

    for r in range(rel):
        for core, values in enumerate(transposed(agg[r * rows : (r + 1) * rows, :])):
            agg_t[r, core] = values
    for core, values in enumerate(transposed(table[:mast, :])):
        self_t[core] = values

    def to_core(src, dst, n):
        return remote(src, dst, s_core.at[n], r_core.at[n], grp_2=1 - c)

    give_agg = to_core(agg_t.at[:, 1 - c], pagg, 0)
    give_self = to_core(self_t.at[1 - c], pself, 1)
    send(give_agg)
    send(give_self)

    def give_masters(h):
        return to_core(gtab.at[h, :mast, :], pgt.at[h, :mast, :], 2 + h)

    def slab_of(b):
        return slice((b % 2) * slab, (b % 2 + 1) * slab)

    def give_mirrors(b):
        some = (b // 2, slice(mast, rows), slab_of(b))
        return to_core(gtab.at[some], pgt.at[some], 4 + b)

    counted(adj_t, source[...], target[...])

    def gpull(b, k):
        at = gtab.at[b // 2, mirror_rows(), pl.ds((b % 2) * slab, slab)]
        return remote(gsend.at[b, zp(k)], at, s_gpull.at[b, k], r_gpull.at[b, k], dom=zp(k))

    for b in range(4):
        for k in ring:
            push(b, k).wait_recv()
        cols = slice(b * slab, (b + 1) * slab)
        part_cols = slice((b % 2) * slab, (b % 2 + 1) * slab)
        value = own[b] + dot(place[...], qrecv[b].reshape(mirrors, slab))
        gate = 1.0 / (1.0 + jnp.exp(-value))
        grad = (cotan[:, cols].astype(F32) * gate * (1.0 + value * (1.0 - gate))).astype(BF16)
        gsend[b] = dot(pick[...], grad).astype(BF16).reshape(nz, cap, slab)
        for k in ring:
            send(gpull(b, k))
        gtab[b // 2, :mast, part_cols] = grad
        gtab[b // 2, mirror_rows(), part_cols] = gsend[b, z]
        act_ref[0, :, cols] = (value * gate).astype(BF16)
        if b % 2:
            send(give_masters(b // 2))

    swapped = rel - 1

    mrow = half // nx

    def block(owner):
        return pl.ds(pl.multiple_of(lax.rem(owner, nx) * mrow, mrow), mrow)

    def along_x(group, i, k):
        lg, xs, xr, ysend, ymine, yr, s_x, r_x, s_y, r_y = group
        to = lax.rem(x + k, nx)
        return remote(xs.at[i, :, block(x + k), :], xr.at[i, k], s_x.at[i, k], r_x.at[i, k], grp_0=to)

    def over_x(group, i):
        lg, xs = group[:2]
        xs[i] = lg[i].astype(BF16)
        for k in nearest_last(nx):
            send(along_x(group, i, k))

    def along_y_first(h, k):
        to = lax.rem(y + k, ny)
        return remote(fs.at[h, :, to], fyr.at[h, k], s_fy.at[h, k], r_fy.at[h, k], grp_1=to)

    def over_y_first(h):
        fs[h] = flg[h].reshape(nx, ny, piece, slab).astype(BF16)
        for k in yring:
            send(along_y_first(h, k))

    def along_x_last(h, k):
        to = lax.rem(x + k, nx)
        return remote(fxs.at[h, to], fxr.at[h, k], s_fx.at[h, k], r_fx.at[h, k], grp_0=to)

    def over_x_last(h):
        for k in yring:
            along_y_first(h, k).wait_recv()
        for owner in range(nx):
            total = flg[h, pl.ds(pl.multiple_of((owner * ny + y) * piece, piece), piece), :]
            for k in yring:
                total += fyr[h, k, owner].astype(F32)
            fmine[h, owner] = total
            fxs[h, owner] = total.astype(BF16)
        for k in nearest_last(nx):
            send(along_x_last(h, k))

    def along_y(group, i, k):
        lg, xs, xr, ysend, ymine, yr, s_x, r_x, s_y, r_y = group
        to = lax.rem(y + k, ny)
        return remote(ysend.at[i, :, to], yr.at[i, k], s_y.at[i, k], r_y.at[i, k], grp_1=to)

    def over_y(group, i):
        lg, xs, xr, ysend, ymine = group[:5]
        for k in range(1, nx):
            along_x(group, i, k).wait_recv()
        for n in range(lg.shape[1]):
            total = lg[i, n, block(x), :]
            for k in range(1, nx):
                total += xr[i, k, n].astype(F32)
            ymine[i, n] = total
            ysend[i, n] = total.reshape(ny, piece, total.shape[1]).astype(BF16)
        for k in yring:
            send(along_y(group, i, k))

    def from_y(group, i):
        ymine, yr = group[4:6]
        for k in yring:
            along_y(group, i, k).wait_recv()
        totals = []
        for n in range(ymine.shape[1]):
            total = ymine[i, n, pl.ds(pl.multiple_of(y * piece, piece), piece), :]
            for k in yring:
                total += yr[i, k, n].astype(F32)
            totals.append(total)
        return totals

    def from_x(b):
        total = fmine[b, x]
        for k in range(1, nx):
            along_x_last(b, k).wait_recv()
            total += fxr[b, k].astype(F32)
        return total

    parts = 5
    held = -(-parts // GROUP)
    owners = nz // GROUP

    def along_z(q, j):
        owner = q % GROUP + j * GROUP
        k = lax.rem(owner - z + 2 * nz, nz)
        return remote(zsend.at[q], zrecv.at[q // GROUP, k], s_z.at[q, j], r_z.at[q // GROUP, k], dom=owner)

    def over_z(q, slabs):
        for n, total in enumerate(slabs):
            zmine[q, n] = total
            zsend[q, n] = total.astype(BF16)
        for j in range(owners):
            @pl.when(z != q % GROUP + j * GROUP)
            def _():
                along_z(q, j).start()

    def shared(i, k):
        q = lax.rem(z, GROUP) + i * GROUP
        return remote(zown.at[i], wrecv.at[q], s_w.at[i, k], r_w.at[q], dom=zp(k))

    near = (2, nz - 1, 1)

    def total_z(i):
        q = lax.rem(z, GROUP) + i * GROUP

        @pl.when(q < parts)
        def _():
            total = zmine[q]
            for k in range(1, nz):
                remote(zsend.at[0], zrecv.at[i, k], s_z.at[0, 0], r_z.at[i, k], dom=zp(1)).wait_recv()
                total += zrecv[i, k].astype(F32)
            zown[i] = total
            for k in near:
                shared(i, k).start()
            wrecv[q] = total

    give_agg.wait_recv()
    give_self.wait_recv()
    for h in (0, 1):
        give_masters(h).wait_recv()
        s_arrays[0][h, 0] = dot(self_t[c], gtab[h, :mast, :]) + dot(pself[...], pgt[h, :mast, :])
        over_x(s_arrays, h)

    wlg = w_arrays[0]
    for b in range(4):
        for k in ring:
            gpull(b, k).wait_recv()
        send(give_mirrors(b))
        flg[b] = dot(agg_t[swapped, c], gtab[b // 2, :, slab_of(b)])
        for r in range(swapped):
            wlg[b, r] = dot(agg_t[r, c], gtab[b // 2, :, slab_of(b)])
        give_mirrors(b).wait_recv()
        flg[b] = flg[b] + dot(pagg[swapped], pgt[b // 2, :, slab_of(b)])
        over_y_first(b)
        for r in range(swapped):
            wlg[b, r] = wlg[b, r] + dot(pagg[r], pgt[b // 2, :, slab_of(b)])
        over_x(w_arrays, b)
        if b == 1:
            over_y(s_arrays, 0)
            over_y(s_arrays, 1)
    over_y(w_arrays, 0)

    for h in (0, 1):
        back[:, h * half : (h + 1) * half] = dot(adj_t[...], gtab[h]).astype(BF16)
    part = dot_nt(back[mast:rows, :], relw[0])
    for r in range(1, rel):
        part += dot_nt(back[r * rows + mast : (r + 1) * rows, :], relw[r])
    bsend[...] = part.astype(BF16).reshape(nz, cap, width)
    brecv[z] = bsend[z]

    def bpush(k):
        return remote(bsend.at[zp(k)], brecv.at[z], s_back.at[k], r_back.at[k], dom=zp(k))

    for k in ring:
        send(bpush(k))

    over_y(w_arrays, 1)
    over_x_last(0)
    over_y(w_arrays, 2)
    over_x_last(1)

    part = dot_nt(gtab[0, :mast, :], selfw[:, :half]) + dot_nt(gtab[1, :mast, :], selfw[:, half:])
    for r in range(rel):
        part += dot_nt(back[r * rows : r * rows + mast, :], relw[r])
    bown[...] = part

    over_y(w_arrays, 3)
    over_z(0, [t[:, i * slab : (i + 1) * slab] for h in (0, 1) for t in from_y(s_arrays, h) for i in (0, 1)])
    over_x_last(2)
    over_x_last(3)
    for b in range(4):
        over_z(1 + b, from_y(w_arrays, b) + [from_x(b)])
    total_z(0)

    for k in ring:
        bpush(k).wait_recv()
    ingrad_ref[0] = (bown[...] + dot(place[...], brecv[...].reshape(mirrors, width))).astype(BF16)

    for i in range(1, held):
        total_z(i)

    for q in range(parts):
        @pl.when(lax.rem(z, GROUP) != q % GROUP)
        def _():
            remote(zown.at[0], wrecv.at[q], s_w.at[0, 1], r_w.at[q], dom=zp(1)).wait_recv()

        for n in range(4):
            r, b = (n, q - 1) if q else (rel, n)
            wgrad_ref[r, :, b * slab : (b + 1) * slab] = wrecv[q, n]

    for copy in sent:
        copy.wait_send()
    for q in range(parts):
        for j in range(owners):
            @pl.when(z != q % GROUP + j * GROUP)
            def _():
                along_z(q, j).wait_send()
    for i in range(held):
        @pl.when(lax.rem(z, GROUP) + i * GROUP < parts)
        def _():
            for k in near:
                shared(i, k).wait_send()


def handed_on(*refs):
    half = len(refs) // 2
    for a, b in zip(refs[:half], refs[half:]):
        b[...] = a[...]


def per_device(
    master_rows, cotangent, relation_weight, self_weight, edge_source, edge_target, edge_relation, send_rows,
    send_counts,
):
    nz = lax.axis_size("dom")
    ny = lax.axis_size("grp_1")
    rel, width = relation_weight.shape[:2]
    mast = master_rows.shape[1]
    mirrors = send_rows.shape[1]
    cap = mirrors // nz
    rows = mast + mirrors
    edges = edge_source.shape[1]
    half = width // 2
    slab = width // 4
    nx = NX
    mrow = half // nx
    piece = width // (nx * ny * 2)
    parts = 5
    held = -(-parts // GROUP)
    vmem = pl.BlockSpec(memory_space=pltpu.VMEM)
    hbm = pl.BlockSpec(memory_space=pl.ANY)
    dma = pltpu.SemaphoreType.DMA

    def summed(units, many, columns):
        return (
            pltpu.VMEM((units, many, half, columns), F32),
            pltpu.VMEM((units, many, half, columns), BF16),
            pltpu.VMEM((units, nx, many, mrow, columns), BF16),
            pltpu.VMEM((units, many, ny, piece, columns), BF16),
            pltpu.VMEM((units, many, mrow, columns), F32),
            pltpu.VMEM((units, ny, many, piece, columns), BF16),
            dma((units, nx)), dma((units, nx)),
            dma((units, ny)), dma((units, ny)),
        )

    scratch = [
        pltpu.SMEM((1, nz), jnp.int32),
        pltpu.VMEM((mast, width), BF16),
        pltpu.VMEM((1, edges), jnp.int32),
        pltpu.VMEM((1, edges), jnp.int32),
        pltpu.VMEM((1, edges), jnp.int32),
        pltpu.VMEM((1, mirrors), jnp.int32),
        pltpu.VMEM((rel, width, width), BF16),
        pltpu.VMEM((width, width), BF16),
        pltpu.VMEM((rows, edges), BF16),
        pltpu.VMEM((rel * rows, rows), BF16),
        pltpu.VMEM((rel * rows, rows), BF16),
        pltpu.VMEM((mast, mirrors), BF16),
        pltpu.VMEM((mirrors, mast), BF16),
        pltpu.VMEM((rows, width), BF16),
        pltpu.VMEM((rel * rows, width), BF16),
        pltpu.VMEM((rel, 2, half, rows), BF16),
        pltpu.VMEM((nz, cap, width), BF16),
        pltpu.VMEM((4, nz, cap, slab), BF16),
        pltpu.VMEM((4, nz, cap, slab), BF16),
        pltpu.VMEM((4, mast, slab), F32),
        pltpu.VMEM((4, nz, cap, slab), BF16),
        pltpu.VMEM((2, rows, half), BF16),
        pltpu.VMEM((rel * rows, width), BF16),
        pltpu.VMEM((mast, width), F32),
        pltpu.VMEM((nz, cap, width), BF16),
        pltpu.VMEM((nz, cap, width), BF16),
        pltpu.VMEM((2, half, mast), BF16),
        pltpu.VMEM((rel, half, rows), BF16),
        pltpu.VMEM((half, mast), BF16),
        pltpu.VMEM((2, rows, half), BF16),
        summed(2, 1, half),
        summed(4, rel - 1, slab),
        pltpu.VMEM((4, half, slab), F32),
        pltpu.VMEM((4, nx, ny, piece, slab), BF16),
        pltpu.VMEM((4, ny, nx, piece, slab), BF16),
        pltpu.VMEM((4, nx, piece, slab), F32),
        pltpu.VMEM((4, nx, piece, slab), BF16),
        pltpu.VMEM((4, nx, piece, slab), BF16),
        pltpu.VMEM((parts, 4, piece, slab), F32),
        pltpu.VMEM((parts, 4, piece, slab), BF16),
        pltpu.VMEM((held, nz, 4, piece, slab), BF16),
        pltpu.VMEM((held, 4, piece, slab), F32),
        pltpu.VMEM((parts, 4, piece, slab), F32),
        dma((9,)),
        dma((nz,)), dma((nz,)),
        dma((4, nz)), dma((4, nz)),
        dma((4, nz)), dma((4, nz)),
        dma((nz,)), dma((nz,)),
        dma((8,)), dma((8,)),
        dma((4, ny)), dma((4, ny)),
        dma((4, nx)), dma((4, nx)),
        dma((parts, nz // GROUP)), dma((held, nz)),
        dma((held, nz)), dma((parts,)),
    ]
    out_shape = (
        jax.ShapeDtypeStruct((1, mast, width), BF16),
        jax.ShapeDtypeStruct((1, mast, width), BF16),
        jax.ShapeDtypeStruct((rel + 1, piece, width), F32),
    )
    results = pl.pallas_call(
        functools.partial(kernel, nz, ny, cap),
        out_shape=tuple(pltpu.VMEM(o.shape, o.dtype) for o in out_shape),
        in_specs=[hbm] * 9,
        out_specs=(vmem, vmem, vmem),
        scratch_shapes=scratch,
        compiler_params=pltpu.CompilerParams(
            collective_id=0, has_side_effects=True, vmem_limit_bytes=56 * 1024 * 1024
        ),
        name="graph_conv_step",
    )(
        send_counts, master_rows, cotangent, edge_source, edge_target, edge_relation, send_rows, relation_weight,
        self_weight,
    )
    return pl.pallas_call(
        handed_on,
        out_shape=out_shape,
        in_specs=[vmem] * 3,
        out_specs=(vmem, vmem, vmem),
        compiler_params=pltpu.CompilerParams(vmem_limit_bytes=4 * 1024 * 1024),
        name="handed_on",
    )(*results)


def solution(mesh):
    devices = mesh.devices.shape[1]
    finer = Mesh(
        mesh.devices.reshape(mesh.shape["dom"], NX, devices // (2 * NX), 2), ("dom", "grp_0", "grp_1", "grp_2")
    )
    in_specs = (
        P(GRP, "dom", None),
        P(GRP, "dom", None),
        P(),
        P(),
        P(GRP, "dom"),
        P(GRP, "dom"),
        P(GRP, "dom"),
        P(GRP, "dom"),
        P(GRP, "dom"),
    )
    out_specs = (P(GRP, "dom", None), P(GRP, "dom", None), P(None, GRP, None))
    return jax.shard_map(per_device, mesh=finer, in_specs=in_specs, out_specs=out_specs, check_vma=False)
```

```python
import functools

import jax
import jax.numpy as jnp
from jax import lax
from jax.experimental import pallas as pl
from jax.experimental.pallas import tpu as pltpu
from jax.sharding import Mesh
from jax.sharding import PartitionSpec as P

GRP = ("grp_0", "grp_1", "grp_2")
MESH = pl.DeviceIdType.MESH
NX = 4
GROUP = 4
F32 = jnp.float32
BF16 = jnp.bfloat16


def dot(a, b):
    return jnp.dot(a, b, preferred_element_type=F32)


def dot_nt(a, b):
    return lax.dot_general(a, b, (((1,), (1,)), ((), ())), preferred_element_type=F32)


def transposed_whole(values):
    return values.astype(F32).T.astype(BF16)


def nearest_last(n):
    return sorted(range(1, n), key=lambda k: (-min(k, n - k), k))


def kernel(
    nz, ny, cap,
    counts_hbm, masters_hbm, cotan_hbm, source_hbm, target_hbm, relation_hbm, slots_hbm, relw_hbm, selfw_hbm,
    act_ref, ingrad_ref, wgrad_ref,
    counts, cotan, source, target, relation, slots, relw, selfw, one_hot, adj, adj_t, place, pick, table, agg, agg_t,
    psend, qsend, qrecv, own, gsend, gtab, back, bown, bsend, brecv, self_t, pagg, pself, pgt, s_arrays, w_arrays,
    flg, fs, fyr, fmine, fxs, fxr, zmine, zsend, zrecv, zown, wrecv,
    in_sem, s_pull, r_pull, s_push, r_push, s_gpull, r_gpull, s_back, r_back, s_core, r_core,
    s_fy, r_fy, s_fx, r_fx, s_z, r_z, s_w, r_w,
):
    z = lax.axis_index("dom")
    x = lax.axis_index("grp_0")
    y = lax.axis_index("grp_1")
    c = lax.axis_index("grp_2")
    nx = NX
    rel = relw.shape[0]
    width = relw.shape[1]
    half = width // 2
    slab = width // 4
    mast = cotan.shape[0]
    rows = table.shape[0]
    mirrors = rows - mast
    piece = width // (nx * ny * 2)
    ring = nearest_last(nz)
    yring = nearest_last(ny)
    sent = []

    def zp(k):
        return lax.rem(z + k, nz)

    def send(copy):
        copy.start()
        sent.append(copy)

    def remote(src, dst, send_sem, recv_sem, **device):
        return pltpu.make_async_remote_copy(
            src_ref=src, dst_ref=dst, send_sem=send_sem, recv_sem=recv_sem, device_id=device, device_id_type=MESH
        )

    barrier = pltpu.get_barrier_semaphore()
    met = [{"dom": zp(k)} for k in ring] + [{"grp_1": lax.rem(y + k, ny)} for k in yring]
    met += [{"grp_0": lax.rem(x + k, nx)} for k in range(1, nx)] + [{"grp_2": 1 - c}]
    for device in met:
        pl.semaphore_signal(barrier, inc=1, device_id=device, device_id_type=MESH)

    brought = (
        (counts_hbm, counts), (slots_hbm, slots), (masters_hbm.at[0], table.at[:mast]), (target_hbm, target),
        (source_hbm, source), (relation_hbm, relation), (relw_hbm, relw), (selfw_hbm, selfw),
        (cotan_hbm.at[0], cotan),
    )
    inputs = [pltpu.make_async_copy(a, b, in_sem.at[i]) for i, (a, b) in enumerate(brought)]
    for copy in inputs:
        copy.start()
    for copy in inputs[:2]:
        copy.wait()

    lane = lax.broadcasted_iota(jnp.int32, (1, mirrors), 1)
    limit = jnp.zeros((1, mirrors), jnp.int32)
    for p in range(nz):
        limit = jnp.where((lane >= p * cap) & (lane < (p + 1) * cap), counts[0, p] + p * cap, limit)
    named = jnp.where(lane < limit, slots[...], -1)
    row = lax.broadcasted_iota(jnp.int32, (mast, mirrors), 0)
    placement = jnp.where(row == named, 1.0, 0.0)
    place[...] = placement.astype(BF16)
    pick[...] = placement.T.astype(BF16)

    inputs[2].wait()
    psend[...] = dot(pick[...], table[:mast, :]).astype(BF16).reshape(nz, cap, width)

    def mirror_rows():
        return pl.ds(pl.multiple_of(mast + z * cap, cap), cap)

    def pull(k):
        return remote(psend.at[zp(k)], table.at[mirror_rows(), :], s_pull.at[k], r_pull.at[k], dom=zp(k))

    pl.semaphore_wait(barrier, len(met))
    for k in ring:
        send(pull(k))
    table[mirror_rows(), :] = psend[z]

    for copy in inputs[3:6]:
        copy.wait()
    row = lax.broadcasted_iota(jnp.int32, (rows, source.shape[1]), 0)

    def counted(dst, first, second):
        one_hot[...] = jnp.where(row == second, 1.0, 0.0).astype(BF16)

        @pl.loop(0, rel)
        def _(r):
            mine = jnp.where(relation[...] == r, first, -1)
            hot = jnp.where(row == mine, 1.0, 0.0).astype(BF16)
            dst[pl.ds(pl.multiple_of(r * rows, rows), rows), :] = dot_nt(hot, one_hot[...]).astype(BF16)

    counted(adj, target[...], source[...])
    for copy in inputs[6:]:
        copy.wait()

    for k in ring:
        pull(k).wait_recv()
    for r in range(rel):
        some = slice(r * rows + mast, (r + 1) * rows)
        agg[some, :] = dot(adj[some, :], table[...]).astype(BF16)

    def push(b, k):
        return remote(qsend.at[b, zp(k)], qrecv.at[b, z], s_push.at[b, k], r_push.at[b, k], dom=zp(k))

    for h in (0, 1):
        cols = slice(h * half, (h + 1) * half)
        part = dot(agg[mast:rows, :], relw[0, :, cols])
        for r in range(1, rel):
            part += dot(agg[r * rows + mast : (r + 1) * rows, :], relw[r, :, cols])
        for b in (2 * h, 2 * h + 1):
            qsend[b] = part[:, (b % 2) * slab : (b % 2 + 1) * slab].astype(BF16).reshape(nz, cap, slab)
            qrecv[b, z] = qsend[b, z]
            for k in ring:
                send(push(b, k))

    for r in range(rel):
        some = slice(r * rows, r * rows + mast)
        agg[some, :] = dot(adj[some, :], table[...]).astype(BF16)

    for h in (0, 1):
        cols = slice(h * half, (h + 1) * half)
        part = dot(table[:mast, :], selfw[:, cols])
        for r in range(rel):
            part += dot(agg[r * rows : r * rows + mast, :], relw[r, :, cols])
        own[2 * h] = part[:, :slab]
        own[2 * h + 1] = part[:, slab:]

    def transposed(values):
        turned = values.astype(F32).T.reshape(nx * ny, 2, piece, values.shape[0])
        return [turned[:, core].reshape(half, values.shape[0]).astype(BF16) for core in (0, 1)]

    for r in range(rel):
        for core, values in enumerate(transposed(agg[r * rows : (r + 1) * rows, :])):
            agg_t[r, core] = values
    for core, values in enumerate(transposed(table[:mast, :])):
        self_t[core] = values

    def to_core(src, dst, n):
        return remote(src, dst, s_core.at[n], r_core.at[n], grp_2=1 - c)

    give_agg = to_core(agg_t.at[:, 1 - c], pagg, 0)
    give_self = to_core(self_t.at[1 - c], pself, 1)
    send(give_agg)
    send(give_self)

    def give_masters(h):
        return to_core(gtab.at[h, :mast, :], pgt.at[h, :mast, :], 2 + h)

    def slab_of(b):
        return slice((b % 2) * slab, (b % 2 + 1) * slab)

    def give_mirrors(b):
        some = (b // 2, slice(mast, rows), slab_of(b))
        return to_core(gtab.at[some], pgt.at[some], 4 + b)

    for r in range(rel):
        adj_t[r * rows : (r + 1) * rows, :] = transposed_whole(adj[r * rows : (r + 1) * rows, :])

    def gpull(b, k):
        at = gtab.at[b // 2, mirror_rows(), pl.ds((b % 2) * slab, slab)]
        return remote(gsend.at[b, zp(k)], at, s_gpull.at[b, k], r_gpull.at[b, k], dom=zp(k))

    for b in range(4):
        for k in ring:
            push(b, k).wait_recv()
        cols = slice(b * slab, (b + 1) * slab)
        part_cols = slice((b % 2) * slab, (b % 2 + 1) * slab)
        value = own[b] + dot(place[...], qrecv[b].reshape(mirrors, slab))
        gate = 1.0 / (1.0 + jnp.exp(-value))
        grad = (cotan[:, cols].astype(F32) * gate * (1.0 + value * (1.0 - gate))).astype(BF16)
        gsend[b] = dot(pick[...], grad).astype(BF16).reshape(nz, cap, slab)
        for k in ring:
            send(gpull(b, k))
        gtab[b // 2, :mast, part_cols] = grad
        gtab[b // 2, mirror_rows(), part_cols] = gsend[b, z]
        act_ref[0, :, cols] = (value * gate).astype(BF16)
        if b % 2:
            send(give_masters(b // 2))

    swapped = rel - 1

    mrow = half // nx

    def block(owner):
        return pl.ds(pl.multiple_of(lax.rem(owner, nx) * mrow, mrow), mrow)

    def along_x(group, i, k):
        lg, xs, xr, ysend, ymine, yr, s_x, r_x, s_y, r_y = group
        to = lax.rem(x + k, nx)
        return remote(xs.at[i, :, block(x + k), :], xr.at[i, k], s_x.at[i, k], r_x.at[i, k], grp_0=to)

    def over_x(group, i):
        lg, xs = group[:2]
        xs[i] = lg[i].astype(BF16)
        for k in nearest_last(nx):
            send(along_x(group, i, k))

    def along_y_first(h, k):
        to = lax.rem(y + k, ny)
        return remote(fs.at[h, :, to], fyr.at[h, k], s_fy.at[h, k], r_fy.at[h, k], grp_1=to)

    def over_y_first(h):
        fs[h] = flg[h].reshape(nx, ny, piece, slab).astype(BF16)
        for k in yring:
            send(along_y_first(h, k))

    def along_x_last(h, k):
        to = lax.rem(x + k, nx)
        return remote(fxs.at[h, to], fxr.at[h, k], s_fx.at[h, k], r_fx.at[h, k], grp_0=to)

    def over_x_last(h):
        for k in yring:
            along_y_first(h, k).wait_recv()
        for owner in range(nx):
            total = flg[h, pl.ds(pl.multiple_of((owner * ny + y) * piece, piece), piece), :]
            for k in yring:
                total += fyr[h, k, owner].astype(F32)
            fmine[h, owner] = total
            fxs[h, owner] = total.astype(BF16)
        for k in nearest_last(nx):
            send(along_x_last(h, k))

    def along_y(group, i, k):
        lg, xs, xr, ysend, ymine, yr, s_x, r_x, s_y, r_y = group
        to = lax.rem(y + k, ny)
        return remote(ysend.at[i, :, to], yr.at[i, k], s_y.at[i, k], r_y.at[i, k], grp_1=to)

    def over_y(group, i):
        lg, xs, xr, ysend, ymine = group[:5]
        for k in range(1, nx):
            along_x(group, i, k).wait_recv()
        for n in range(lg.shape[1]):
            total = lg[i, n, block(x), :]
            for k in range(1, nx):
                total += xr[i, k, n].astype(F32)
            ymine[i, n] = total
            ysend[i, n] = total.reshape(ny, piece, total.shape[1]).astype(BF16)
        for k in yring:
            send(along_y(group, i, k))

    def from_y(group, i):
        ymine, yr = group[4:6]
        for k in yring:
            along_y(group, i, k).wait_recv()
        totals = []
        for n in range(ymine.shape[1]):
            total = ymine[i, n, pl.ds(pl.multiple_of(y * piece, piece), piece), :]
            for k in yring:
                total += yr[i, k, n].astype(F32)
            totals.append(total)
        return totals

    def from_x(b):
        total = fmine[b, x]
        for k in range(1, nx):
            along_x_last(b, k).wait_recv()
            total += fxr[b, k].astype(F32)
        return total

    parts = 5
    held = -(-parts // GROUP)
    owners = nz // GROUP

    def along_z(q, j):
        owner = q % GROUP + j * GROUP
        k = lax.rem(owner - z + 2 * nz, nz)
        return remote(zsend.at[q], zrecv.at[q // GROUP, k], s_z.at[q, j], r_z.at[q // GROUP, k], dom=owner)

    def over_z(q, slabs):
        for n, total in enumerate(slabs):
            zmine[q, n] = total
            zsend[q, n] = total.astype(BF16)
        for j in range(owners):
            @pl.when(z != q % GROUP + j * GROUP)
            def _():
                along_z(q, j).start()

    def shared(i, k):
        q = lax.rem(z, GROUP) + i * GROUP
        return remote(zown.at[i], wrecv.at[q], s_w.at[i, k], r_w.at[q], dom=zp(k))

    near = (2, nz - 1, 1)

    def total_z(i):
        q = lax.rem(z, GROUP) + i * GROUP

        @pl.when(q < parts)
        def _():
            total = zmine[q]
            for k in range(1, nz):
                remote(zsend.at[0], zrecv.at[i, k], s_z.at[0, 0], r_z.at[i, k], dom=zp(1)).wait_recv()
                total += zrecv[i, k].astype(F32)
            zown[i] = total
            for k in near:
                shared(i, k).start()
            wrecv[q] = total

    give_agg.wait_recv()
    give_self.wait_recv()
    for h in (0, 1):
        give_masters(h).wait_recv()
        s_arrays[0][h, 0] = dot(self_t[c], gtab[h, :mast, :]) + dot(pself[...], pgt[h, :mast, :])
        over_x(s_arrays, h)

    wlg = w_arrays[0]
    for b in range(4):
        for k in ring:
            gpull(b, k).wait_recv()
        send(give_mirrors(b))
        flg[b] = dot(agg_t[swapped, c], gtab[b // 2, :, slab_of(b)])
        for r in range(swapped):
            wlg[b, r] = dot(agg_t[r, c], gtab[b // 2, :, slab_of(b)])
        give_mirrors(b).wait_recv()
        flg[b] = flg[b] + dot(pagg[swapped], pgt[b // 2, :, slab_of(b)])
        over_y_first(b)
        for r in range(swapped):
            wlg[b, r] = wlg[b, r] + dot(pagg[r], pgt[b // 2, :, slab_of(b)])
        over_x(w_arrays, b)
        if b == 1:
            over_y(s_arrays, 0)
            over_y(s_arrays, 1)
    over_y(w_arrays, 0)

    for h in (0, 1):
        back[:, h * half : (h + 1) * half] = dot(adj_t[...], gtab[h]).astype(BF16)
    over_y(w_arrays, 1)
    part = dot_nt(back[mast:rows, :], relw[0])
    for r in range(1, rel):
        part += dot_nt(back[r * rows + mast : (r + 1) * rows, :], relw[r])
    bsend[...] = part.astype(BF16).reshape(nz, cap, width)
    brecv[z] = bsend[z]

    def bpush(k):
        return remote(bsend.at[zp(k)], brecv.at[z], s_back.at[k], r_back.at[k], dom=zp(k))

    for k in ring:
        send(bpush(k))

    over_x_last(0)
    over_y(w_arrays, 2)
    over_x_last(1)

    part = dot_nt(gtab[0, :mast, :], selfw[:, :half]) + dot_nt(gtab[1, :mast, :], selfw[:, half:])
    for r in range(rel):
        part += dot_nt(back[r * rows : r * rows + mast, :], relw[r])
    bown[...] = part

    over_y(w_arrays, 3)
    over_z(0, [t[:, i * slab : (i + 1) * slab] for h in (0, 1) for t in from_y(s_arrays, h) for i in (0, 1)])
    over_x_last(2)
    over_x_last(3)
    for b in range(4):
        over_z(1 + b, from_y(w_arrays, b) + [from_x(b)])
    total_z(0)

    for k in ring:
        bpush(k).wait_recv()
    ingrad_ref[0] = (bown[...] + dot(place[...], brecv[...].reshape(mirrors, width))).astype(BF16)

    for i in range(1, held):
        total_z(i)

    for q in range(parts):
        @pl.when(lax.rem(z, GROUP) != q % GROUP)
        def _():
            remote(zown.at[0], wrecv.at[q], s_w.at[0, 1], r_w.at[q], dom=zp(1)).wait_recv()

        for n in range(4):
            r, b = (n, q - 1) if q else (rel, n)
            wgrad_ref[r, :, b * slab : (b + 1) * slab] = wrecv[q, n]

    for copy in sent:
        copy.wait_send()
    for q in range(parts):
        for j in range(owners):
            @pl.when(z != q % GROUP + j * GROUP)
            def _():
                along_z(q, j).wait_send()
    for i in range(held):
        @pl.when(lax.rem(z, GROUP) + i * GROUP < parts)
        def _():
            for k in near:
                shared(i, k).wait_send()


def handed_on(*refs):
    half = len(refs) // 2
    for a, b in zip(refs[:half], refs[half:]):
        b[...] = a[...]


def per_device(
    master_rows, cotangent, relation_weight, self_weight, edge_source, edge_target, edge_relation, send_rows,
    send_counts,
):
    nz = lax.axis_size("dom")
    ny = lax.axis_size("grp_1")
    rel, width = relation_weight.shape[:2]
    mast = master_rows.shape[1]
    mirrors = send_rows.shape[1]
    cap = mirrors // nz
    rows = mast + mirrors
    edges = edge_source.shape[1]
    half = width // 2
    slab = width // 4
    nx = NX
    mrow = half // nx
    piece = width // (nx * ny * 2)
    parts = 5
    held = -(-parts // GROUP)
    vmem = pl.BlockSpec(memory_space=pltpu.VMEM)
    hbm = pl.BlockSpec(memory_space=pl.ANY)
    dma = pltpu.SemaphoreType.DMA

    def summed(units, many, columns):
        return (
            pltpu.VMEM((units, many, half, columns), F32),
            pltpu.VMEM((units, many, half, columns), BF16),
            pltpu.VMEM((units, nx, many, mrow, columns), BF16),
            pltpu.VMEM((units, many, ny, piece, columns), BF16),
            pltpu.VMEM((units, many, mrow, columns), F32),
            pltpu.VMEM((units, ny, many, piece, columns), BF16),
            dma((units, nx)), dma((units, nx)),
            dma((units, ny)), dma((units, ny)),
        )

    scratch = [
        pltpu.SMEM((1, nz), jnp.int32),
        pltpu.VMEM((mast, width), BF16),
        pltpu.VMEM((1, edges), jnp.int32),
        pltpu.VMEM((1, edges), jnp.int32),
        pltpu.VMEM((1, edges), jnp.int32),
        pltpu.VMEM((1, mirrors), jnp.int32),
        pltpu.VMEM((rel, width, width), BF16),
        pltpu.VMEM((width, width), BF16),
        pltpu.VMEM((rows, edges), BF16),
        pltpu.VMEM((rel * rows, rows), BF16),
        pltpu.VMEM((rel * rows, rows), BF16),
        pltpu.VMEM((mast, mirrors), BF16),
        pltpu.VMEM((mirrors, mast), BF16),
        pltpu.VMEM((rows, width), BF16),
        pltpu.VMEM((rel * rows, width), BF16),
        pltpu.VMEM((rel, 2, half, rows), BF16),
        pltpu.VMEM((nz, cap, width), BF16),
        pltpu.VMEM((4, nz, cap, slab), BF16),
        pltpu.VMEM((4, nz, cap, slab), BF16),
        pltpu.VMEM((4, mast, slab), F32),
        pltpu.VMEM((4, nz, cap, slab), BF16),
        pltpu.VMEM((2, rows, half), BF16),
        pltpu.VMEM((rel * rows, width), BF16),
        pltpu.VMEM((mast, width), F32),
        pltpu.VMEM((nz, cap, width), BF16),
        pltpu.VMEM((nz, cap, width), BF16),
        pltpu.VMEM((2, half, mast), BF16),
        pltpu.VMEM((rel, half, rows), BF16),
        pltpu.VMEM((half, mast), BF16),
        pltpu.VMEM((2, rows, half), BF16),
        summed(2, 1, half),
        summed(4, rel - 1, slab),
        pltpu.VMEM((4, half, slab), F32),
        pltpu.VMEM((4, nx, ny, piece, slab), BF16),
        pltpu.VMEM((4, ny, nx, piece, slab), BF16),
        pltpu.VMEM((4, nx, piece, slab), F32),
        pltpu.VMEM((4, nx, piece, slab), BF16),
        pltpu.VMEM((4, nx, piece, slab), BF16),
        pltpu.VMEM((parts, 4, piece, slab), F32),
        pltpu.VMEM((parts, 4, piece, slab), BF16),
        pltpu.VMEM((held, nz, 4, piece, slab), BF16),
        pltpu.VMEM((held, 4, piece, slab), F32),
        pltpu.VMEM((parts, 4, piece, slab), F32),
        dma((9,)),
        dma((nz,)), dma((nz,)),
        dma((4, nz)), dma((4, nz)),
        dma((4, nz)), dma((4, nz)),
        dma((nz,)), dma((nz,)),
        dma((8,)), dma((8,)),
        dma((4, ny)), dma((4, ny)),
        dma((4, nx)), dma((4, nx)),
        dma((parts, nz // GROUP)), dma((held, nz)),
        dma((held, nz)), dma((parts,)),
    ]
    out_shape = (
        jax.ShapeDtypeStruct((1, mast, width), BF16),
        jax.ShapeDtypeStruct((1, mast, width), BF16),
        jax.ShapeDtypeStruct((rel + 1, piece, width), F32),
    )
    results = pl.pallas_call(
        functools.partial(kernel, nz, ny, cap),
        out_shape=tuple(pltpu.VMEM(o.shape, o.dtype) for o in out_shape),
        in_specs=[hbm] * 9,
        out_specs=(vmem, vmem, vmem),
        scratch_shapes=scratch,
        compiler_params=pltpu.CompilerParams(
            collective_id=0, has_side_effects=True, vmem_limit_bytes=56 * 1024 * 1024
        ),
        name="graph_conv_step",
    )(
        send_counts, master_rows, cotangent, edge_source, edge_target, edge_relation, send_rows, relation_weight,
        self_weight,
    )
    return pl.pallas_call(
        handed_on,
        out_shape=out_shape,
        in_specs=[vmem] * 3,
        out_specs=(vmem, vmem, vmem),
        compiler_params=pltpu.CompilerParams(vmem_limit_bytes=4 * 1024 * 1024),
        name="handed_on",
    )(*results)


def solution(mesh):
    devices = mesh.devices.shape[1]
    finer = Mesh(
        mesh.devices.reshape(mesh.shape["dom"], NX, devices // (2 * NX), 2), ("dom", "grp_0", "grp_1", "grp_2")
    )
    in_specs = (
        P(GRP, "dom", None),
        P(GRP, "dom", None),
        P(),
        P(),
        P(GRP, "dom"),
        P(GRP, "dom"),
        P(GRP, "dom"),
        P(GRP, "dom"),
        P(GRP, "dom"),
    )
    out_specs = (P(GRP, "dom", None), P(GRP, "dom", None), P(None, GRP, None))
    return jax.shard_map(per_device, mesh=finer, in_specs=in_specs, out_specs=out_specs, check_vma=False)
```
